32 devices in a mesh: dp: 8 (over z, y), mp: 4 (over x, core).
Axes of the slice: x: 2, y: 2, z: 4, core: 2. Of those that a mesh axis runs over, the one named last changes fastest.
Arguments:
- tokens: bfloat16 [8192, 4096], P('dp', 'mp'), may hold values from -6 to 6
- right_weight: bfloat16 [64, 64, 64], P('mp', 'dp'), may hold values from -0.75 to 0.75
- left_weight: bfloat16 [64, 64, 64], P('mp', 'dp'), may hold values from -0.75 to 0.75
- cotangent: bfloat16 [8192, 4096], P('dp', 'mp'), may hold values from -0.06591797 to 0.06591797
Outputs:
- activated: bfloat16 [8192, 4096], P('dp', 'mp')
- grad_right: float32 [64, 64, 64], P('mp', 'dp')
- grad_left: float32 [64, 64, 64], P('mp', 'dp')
The draws below stay inside these ranges and needn't reach their ends.
All inputs are finite; a program needn't handle non-finite values.
Results may differ from the reference program's by a relative error of at most 0.0056.
Values may be sent and summed in bfloat16 or wider, within the bound.
A program may use at most 64 MiB of HBM per device.

```python
import jax
import jax.numpy as jnp
from jax import lax

NB = 64
BS = 64
TOK_DEV = 1024
D = 4096
TOKENS = 8192
N_DP = 8


def block_scale(rng, dims, cuts, smallest, top_value):
    loudness, own = 1.0, jax.random.fold_in(rng, 6)
    for dim, shards_of in cuts:
        heights = jnp.exp(jax.random.uniform(jax.random.fold_in(own, dim), (shards_of,), jnp.float32, smallest / len(cuts), top_value / len(cuts)))
        loudness = loudness * jnp.repeat(heights, dims[dim] // shards_of).reshape([-1 if axis == dim else 1 for axis in range(len(dims))])
    return loudness


def scatter_about(rng, dims, width, limit, shards=(), dtype=jnp.bfloat16):
    result = width * jax.random.normal(rng, dims, jnp.float32)
    if shards:
        result = result * block_scale(rng, dims, shards, -0.22, 0.18)
    return jnp.clip(result, -limit, limit).astype(dtype)


def setup_inputs(seed: int = 0) -> dict:
    keys = jax.random.split(jax.random.key(seed), 5)
    return {
        "tokens": scatter_about(keys[0], (TOKENS, D), 1.0, 6.0, ((0, 8), (1, 4))),
        "right_weight": scatter_about(keys[1], (NB, BS, BS), BS ** -0.5, 0.75, ((0, 4), (1, 8))),
        "left_weight": scatter_about(keys[2], (BS, NB, BS), NB ** -0.5, 0.75, ((0, 4), (1, 8))),
        "cotangent": scatter_about(keys[3], (TOKENS, D), ((TOK_DEV * N_DP) ** -0.5), 0.06591797, ((0, 8), (1, 4))),
    }


def gelu_slope(pre):
    cdf = 0.5 * (1.0 + lax.erf(pre * 0.7071067811865476))
    density = jnp.exp(-0.5 * pre * pre) * 0.3989422804014327
    return cdf + pre * density


def reference(tokens, right_weight, left_weight, cotangent):
    right_f = right_weight.astype(jnp.float32)
    left_f = left_weight.astype(jnp.float32)
    xs_all = tokens.reshape(N_DP, TOK_DEV, NB, BS)
    gs_all = cotangent.reshape(N_DP, TOK_DEV, BS, BS)

    def step(carry, pieces):
        grad_r, grad_l = carry
        xs, gs = pieces
        xs_f = xs.astype(jnp.float32)
        inner = jnp.einsum('tik,ikm->tim', xs_f, right_f).astype(jnp.bfloat16)
        inner_f = inner.astype(jnp.float32)
        pre = jnp.einsum('tim,min->tmn', inner_f, left_f)
        activated = jax.nn.gelu(pre, approximate=False).astype(jnp.bfloat16)
        dpre = (gs.astype(jnp.float32) * gelu_slope(pre)).astype(jnp.bfloat16)
        dpre_f = dpre.astype(jnp.float32)
        grad_l = grad_l + jnp.einsum('tim,tmn->min', inner_f, dpre_f)
        dinner = jnp.einsum('tmn,min->tim', dpre_f, left_f).astype(jnp.bfloat16)
        grad_r = grad_r + jnp.einsum('tik,tim->ikm', xs_f, dinner.astype(jnp.float32))
        return (grad_r, grad_l), activated

    start = (jnp.zeros((NB, BS, BS), jnp.float32), jnp.zeros((BS, NB, BS), jnp.float32))
    (grad_right, grad_left), outs = lax.scan(step, start, (xs_all, gs_all))
    activated = outs.reshape(N_DP * TOK_DEV, NB * BS)
    return activated, grad_right, grad_left
```

```python
import functools

import jax
import jax.numpy as jnp
from jax import lax
from jax.experimental import pallas as pl
from jax.experimental.pallas import tpu as pltpu
from jax.sharding import PartitionSpec as P

MESH = pl.DeviceIdType.MESH
BF = jnp.bfloat16
F32 = jnp.float32
CHUNKS = 8
TAIL = (1,)


def iota(shape, dim):
    line = tuple(n if axis == dim else 1 for axis, n in enumerate(shape))
    return lax.broadcasted_iota(jnp.int32, line, dim)


def ones_where(cond):
    return jnp.where(cond, 1.0, 0.0).astype(BF)


def dot_nn(a, b):
    return lax.dot_general(a, b, (((1,), (0,)), ((), ())), preferred_element_type=F32)


def dot_nt(a, b):
    return lax.dot_general(a, b, (((1,), (1,)), ((), ())), preferred_element_type=F32)


def dot_tn(a, b):
    return lax.dot_general(a, b, (((0,), (0,)), ((), ())), preferred_element_type=F32)


def join(parts, axis=1):
    return parts[0] if len(parts) == 1 else jnp.concatenate(parts, axis=axis)


def across(index, r):
    bit = 1 << r
    return index + bit - 2 * bit * lax.rem(index // bit, 2)


class Sizes:
    def __init__(self, n_dp, n_mp, tok_rows, features, width):
        self.dp, self.mp = n_dp, n_mp
        self.tok, self.feat, self.bs = tok_rows, features, width
        self.own = features // width
        self.blocks = self.own * n_mp
        self.rows = width // n_dp
        self.orow = self.own * self.rows
        self.pad = max(self.own, 16)
        self.gs = max(1, 128 // (self.own * self.own))
        self.groups = n_mp // self.gs
        self.ng = self.gs * self.own * self.own
        self.kg = self.gs * features
        self.jg = self.ng // 128
        self.jl = self.own // self.jg
        self.nj = self.ng // self.jg
        self.rh = self.groups * self.nj
        self.fj = self.jl * width
        self.n = n_dp * n_mp
        self.direct = self.pad == self.own and self.orow % 128 == 0
        self.tc = tok_rows // CHUNKS
        self.main = CHUNKS - 1
        self.tail = []
        start = self.main * self.tc
        for part in TAIL:
            self.tail.append((self.main + len(self.tail), start, self.tc // part))
            start += self.tc // part
        self.parts = self.main + len(self.tail)
        self.rounds = n_dp.bit_length() - 1
        self.cube = n_dp == 1 << self.rounds


def kernel(z, x_hbm, cot_hbm, rw_hbm, lw_hbm, act, gr_ref, gl_ref,
           xfull, cot, rw_v, lw_v, rwt, lwt, rg, lg, p1, p2, wt, lt, gracc, glacc,
           rsend, rrecv, lsend, lrecv,
           x_recv, x_send, x_local, c_local, w_local,
           rw_send, rw_recv, lw_send, lw_recv, gr_send, gr_recv, gl_send, gl_recv, ra_send, ra_recv, met):
    d, p = lax.axis_index("dp"), lax.axis_index("mp")
    me = d * z.mp + p
    core = lax.rem(p, 2)
    partner = p + 1 - 2 * core
    chip = p // 2
    chips = z.mp // 2

    def same_core(s):
        return lax.rem(chip + s, chips) * 2 + core

    def other_core(s):
        return lax.rem(chip + s, chips) * 2 + 1 - core

    barrier = pltpu.get_barrier_semaphore()
    if z.cube:
        for s in range(1, z.mp):
            pl.semaphore_signal(barrier, inc=1, device_id=(d, lax.rem(p + s, z.mp)), device_id_type=MESH)
        for r in range(z.rounds):
            pl.semaphore_signal(barrier, inc=1, device_id=(across(d, r), p), device_id_type=MESH)
        near = z.mp - 1 + z.rounds
    else:
        @pl.loop(1, z.n)
        def _(s):
            o = lax.rem(me + s, z.n)
            pl.semaphore_signal(barrier, inc=1, device_id=(o // z.mp, lax.rem(o, z.mp)), device_id_type=MESH)
        near = z.n - 1

    def full(c):
        return c, pl.multiple_of(c * z.tc, z.tc), z.tc

    def local_x(part):
        c, start, size = part
        return pltpu.make_async_copy(x_hbm.at[pl.ds(start, size)], xfull.at[p, pl.ds(start, size)], x_local.at[c])

    def local_c(part):
        c, start, size = part
        return pltpu.make_async_copy(cot_hbm.at[pl.ds(start, size)], cot.at[pl.ds(start, size)], c_local.at[c])

    def send_own(part, kind, target):
        c, start, size = part
        return pltpu.make_async_remote_copy(
            src_ref=x_hbm.at[pl.ds(start, size)], dst_ref=xfull.at[p, pl.ds(start, size)],
            send_sem=x_send.at[kind, c], recv_sem=x_recv.at[p, c],
            device_id=(d, target), device_id_type=MESH)

    def forward(part, kind, source):
        c, start, size = part
        return pltpu.make_async_remote_copy(
            src_ref=xfull.at[source, pl.ds(start, size)], dst_ref=xfull.at[source, pl.ds(start, size)],
            send_sem=x_send.at[kind, c], recv_sem=x_recv.at[source, c],
            device_id=(d, partner), device_id_type=MESH)

    def arrived(part, source):
        c, start, size = part
        pltpu.make_async_remote_copy(
            src_ref=xfull.at[source, pl.ds(start, size)], dst_ref=xfull.at[source, pl.ds(start, size)],
            send_sem=x_send.at[0, c], recv_sem=x_recv.at[source, c],
            device_id=(d, partner), device_id_type=MESH).wait_recv()

    def each_part(step, first=0):
        @pl.loop(first, z.main)
        def _(c):
            step(full(c))
        for part in z.tail:
            step(part)

    local_r = pltpu.make_async_copy(rw_hbm, rw_v, w_local.at[0])
    local_r.start()
    local_l = pltpu.make_async_copy(lw_hbm, lw_v, w_local.at[1])
    local_l.start()

    local_r.wait()
    local_l.wait()
    shape = (z.mp * z.pad, z.bs)
    a, b = iota(shape, 0), iota(shape, 1)
    wide = ones_where((a % z.pad < z.own) & (b == (a // z.pad) * z.own + a % z.pad))
    rwt[...] = dot_nt(wide, rw_v[...]).astype(BF).reshape(z.mp, z.pad, z.orow)
    shape = (z.bs, z.bs)
    lwt[...] = dot_nt(ones_where(iota(shape, 0) == iota(shape, 1)), lw_v[...]).astype(BF)
    rg[me] = rwt[p]
    lg[d] = lwt[...]

    pl.semaphore_wait(barrier, near)

    def send_x(part):
        for s in range(1, chips):
            send_own(part, s, same_core(s)).start()
        send_own(part, 0, partner).start()

    for s in range(1, z.mp):
        q = lax.rem(p + s, z.mp)
        pltpu.make_async_remote_copy(
            src_ref=rwt.at[q], dst_ref=rg.at[me], send_sem=ra_send, recv_sem=ra_recv,
            device_id=(d, q), device_id_type=MESH).start()

    each_part(send_x)

    if z.cube:
        for r in range(z.rounds):
            pl.semaphore_signal(met.at[r], inc=1, device_id=(across(d, r), p), device_id_type=MESH)
            pl.semaphore_wait(met.at[r], 1)

    @each_part
    def _(part):
        local_x(part).start()
        local_c(part).start()

    def count(ref, sem):
        pltpu.make_async_copy(ref, ref, sem).wait()

    @pl.loop(1, z.dp)
    def _(s):
        pltpu.make_async_remote_copy(
            src_ref=lwt, dst_ref=lg.at[d], send_sem=lw_send, recv_sem=lw_recv,
            device_id=(lax.rem(d + s, z.dp), p), device_id_type=MESH).start()

    count(rg.at[pl.ds(0, z.mp - 1)], ra_recv)
    mine = rg.at[pl.ds(d * z.mp, z.mp)]

    @pl.loop(1, z.dp)
    def _(s):
        pltpu.make_async_remote_copy(
            src_ref=mine, dst_ref=mine, send_sem=rw_send, recv_sem=rw_recv,
            device_id=(lax.rem(d + s, z.dp), p), device_id_type=MESH).start()

    for dd in range(z.dp):
        shape = (z.orow, z.feat)
        a, b = iota(shape, 0), iota(shape, 1)
        source = (b // z.bs) * z.rows + (b % z.bs) - dd * z.rows
        inside = (b % z.bs) // z.rows == dd
        p1[dd] = ones_where(inside & (a == source))
        shape = (z.orow, z.blocks * z.own)
        a, b = iota(shape, 0), iota(shape, 1)
        jg = b // z.rh
        i_all = (b % z.rh) // z.jl
        j = jg * z.jl + b % z.jl
        inside = i_all // z.rows == dd
        p2[dd] = ones_where(inside & (a == j * z.rows + i_all % z.rows))
    gracc[...] = jnp.zeros_like(gracc)
    glacc[...] = jnp.zeros_like(glacc)

    count(lg.at[pl.ds(0, z.dp - 1)], lw_recv)
    left = None
    for dd in range(z.dp):
        part = dot_nn(lg[dd], p2[dd])
        left = part if left is None else left + part
    left = left.astype(BF)
    shape = (z.fj, z.bs)
    spread = ones_where(iota(shape, 0) % z.bs == iota(shape, 1))
    for jg in range(z.jg):
        piece = dot_nn(spread, left[:, jg * z.rh:(jg + 1) * z.rh])
        keep = iota((z.fj, z.rh), 0) // z.bs == iota((z.fj, z.rh), 1) % z.jl
        lt[jg] = jnp.where(keep, piece, 0.0).astype(BF)

    count(rg.at[pl.ds(0, z.n - z.mp)], rw_recv)
    right = None
    for dd in range(z.dp):
        part = dot_nn(rg[dd * z.mp:(dd + 1) * z.mp].reshape(z.mp * z.pad, z.orow), p1[dd])
        right = part if right is None else right + part
    right = right.astype(BF)
    for g in range(z.groups):
        for s in range(z.gs):
            shape = (z.ng, z.mp * z.pad)
            a, b = iota(shape, 0), iota(shape, 1)
            j = (a // z.nj) * z.jl + a % z.jl
            src = (a % z.nj) // (z.own * z.jl)
            pick = ones_where((src == s) & (b == (g * z.gs + s) * z.pad + j))
            piece = dot_nn(pick, right)
            shape = (z.ng, z.feat)
            keep = (iota(shape, 0) // z.jl) % z.own == iota(shape, 1) // z.bs
            wt[g, :, s * z.feat:(s + 1) * z.feat] = jnp.where(keep, piece, 0.0).astype(BF)

    @each_part
    def _(part):
        local_x(part).wait()
        local_c(part).wait()
        for s in range(1, chips):
            arrived(part, same_core(s))
            forward(part, chips + s, same_core(s)).start()
        arrived(part, partner)
        for s in range(1, chips):
            arrived(part, other_core(s))
        r = pl.ds(part[1], part[2])
        xs = [join([xfull[g * z.gs + s, r] for s in range(z.gs)]) for g in range(z.groups)]
        inner = [dot_nt(xs[g], wt[g]).astype(BF) for g in range(z.groups)]
        back = []
        for jg in range(z.jg):
            mixed = join([v[:, jg * z.nj:(jg + 1) * z.nj] for v in inner])
            pre = dot_nt(mixed, lt[jg])
            cdf = 0.5 * (1.0 + lax.erf(pre * 0.7071067811865476))
            slope = cdf + pre * (jnp.exp(-0.5 * pre * pre) * 0.3989422804014327)
            cols = pl.ds(jg * z.fj, z.fj)
            act[r, cols] = (pre * cdf).astype(BF)
            dpre = (cot[r, cols].astype(F32) * slope).astype(BF)
            glacc[jg] += dot_tn(dpre, mixed)
            back.append(dot_nn(dpre, lt[jg]).astype(BF))
        for g in range(z.groups):
            dinner = join([v[:, g * z.nj:(g + 1) * z.nj] for v in back])
            gracc[g] += dot_tn(dinner, xs[g])

    shape = (z.bs, z.fj)
    fold = ones_where(iota(shape, 1) % z.bs == iota(shape, 0))
    lefts = []
    for jg in range(z.jg):
        keep = iota((z.fj, z.rh), 0) // z.bs == iota((z.fj, z.rh), 1) % z.jl
        lefts.append(dot_nn(fold, jnp.where(keep, glacc[jg], 0.0).astype(BF)).astype(BF))
    left = join(lefts)
    for dd in range(z.dp):
        lsend[dd] = dot_nt(left, p2[dd]).astype(BF)

    @pl.loop(1, z.dp)
    def _(s):
        o = lax.rem(d + s, z.dp)
        pltpu.make_async_remote_copy(
            src_ref=lsend.at[o], dst_ref=lrecv.at[d], send_sem=gl_send, recv_sem=gl_recv,
            device_id=(o, p), device_id_type=MESH).start()

    pieces = []
    for g in range(z.groups):
        for s in range(z.gs):
            shape = (z.pad, z.ng)
            a, b = iota(shape, 0), iota(shape, 1)
            j = (b // z.nj) * z.jl + b % z.jl
            src = (b % z.nj) // (z.own * z.jl)
            pick = ones_where((src == s) & (a == j))
            shape = (z.ng, z.feat)
            keep = (iota(shape, 0) // z.jl) % z.own == iota(shape, 1) // z.bs
            piece = jnp.where(keep, gracc[g, :, s * z.feat:(s + 1) * z.feat], 0.0).astype(BF)
            pieces.append(dot_nn(pick, piece).astype(BF))
    pieces = join(pieces, axis=0)
    for dd in range(z.dp):
        owned = dot_nt(pieces, p1[dd]).astype(BF)
        rsend[dd * z.mp:(dd + 1) * z.mp] = owned.reshape(z.mp, z.pad, z.orow)

    @pl.loop(1, z.n)
    def _(s):
        o = lax.rem(me + s, z.n)
        pltpu.make_async_remote_copy(
            src_ref=rsend.at[o], dst_ref=rrecv.at[me], send_sem=gr_send, recv_sem=gr_recv,
            device_id=(o // z.mp, lax.rem(o, z.mp)), device_id_type=MESH).start()

    lrecv[d] = lsend[d]
    rrecv[me] = rsend[me]

    @each_part
    def _(part):
        for s in range(1, chips):
            send_own(part, s, same_core(s)).wait_send()
            forward(part, chips + s, same_core(s)).wait_send()
        send_own(part, 0, partner).wait_send()

    count(rg.at[pl.ds(0, z.mp - 1)], ra_send)
    count(rg.at[pl.ds(0, z.n - z.mp)], rw_send)
    count(lg.at[pl.ds(0, z.dp - 1)], lw_send)

    count(lrecv.at[pl.ds(0, z.dp - 1)], gl_recv)
    total = lrecv[0].astype(F32)
    for dd in range(1, z.dp):
        total = total + lrecv[dd].astype(F32)
    gl_ref[...] = total.T if z.direct else total
    count(rrecv.at[pl.ds(0, z.n - 1)], gr_recv)
    total = rrecv[0:z.mp].astype(F32)
    for dd in range(1, z.dp):
        total = total + rrecv[dd * z.mp:(dd + 1) * z.mp].astype(F32)
    gr_ref[...] = total.reshape(z.blocks, z.orow).T if z.direct else total
    count(lsend.at[pl.ds(0, z.dp - 1)], gl_send)
    count(rsend.at[pl.ds(0, z.n - 1)], gr_send)


def store(*refs):
    sems = refs[6]
    copies = [pltpu.make_async_copy(refs[k], refs[k + 3], sems.at[k]) for k in range(3)]
    for copy in copies:
        copy.start()
    for copy in copies:
        copy.wait()


def shards(z, tokens, right_weight, left_weight, cotangent):
    rw = right_weight.reshape(z.orow, z.bs)
    lw = left_weight.reshape(z.orow, z.bs)
    hbm = pl.BlockSpec(memory_space=pltpu.HBM)
    vmem = pl.BlockSpec(memory_space=pltpu.VMEM)
    dma = pltpu.SemaphoreType.DMA
    act, gr, gl = pl.pallas_call(
        functools.partial(kernel, z),
        out_shape=(
            pltpu.VMEM((z.tok, z.feat), BF),
            pltpu.VMEM((z.orow, z.bs) if z.direct else (z.mp, z.pad, z.orow), F32),
            pltpu.VMEM((z.orow, z.bs) if z.direct else (z.bs, z.orow), F32),
        ),
        in_specs=[hbm] * 4,
        out_specs=(vmem, vmem, vmem),
        scratch_shapes=[
            pltpu.VMEM((z.mp, z.tok, z.feat), BF),
            pltpu.VMEM((z.tok, z.feat), BF),
            pltpu.VMEM((z.orow, z.bs), BF),
            pltpu.VMEM((z.orow, z.bs), BF),
            pltpu.VMEM((z.mp, z.pad, z.orow), BF),
            pltpu.VMEM((z.bs, z.orow), BF),
            pltpu.VMEM((z.n, z.pad, z.orow), BF),
            pltpu.VMEM((z.dp, z.bs, z.orow), BF),
            pltpu.VMEM((z.dp, z.orow, z.feat), BF),
            pltpu.VMEM((z.dp, z.orow, z.blocks * z.own), BF),
            pltpu.VMEM((z.groups, z.ng, z.kg), BF),
            pltpu.VMEM((z.jg, z.fj, z.rh), BF),
            pltpu.VMEM((z.groups, z.ng, z.kg), F32),
            pltpu.VMEM((z.jg, z.fj, z.rh), F32),
            pltpu.VMEM((z.n, z.pad, z.orow), BF),
            pltpu.VMEM((z.n, z.pad, z.orow), BF),
            pltpu.VMEM((z.dp, z.bs, z.orow), BF),
            pltpu.VMEM((z.dp, z.bs, z.orow), BF),
            dma((z.mp, z.parts)),
            dma((z.mp, z.parts)),
            dma((z.parts,)),
            dma((z.parts,)),
            dma((2,)),
            dma, dma, dma, dma, dma, dma, dma, dma, dma, dma,
            pltpu.SemaphoreType.REGULAR((max(1, z.rounds),)),
        ],
        compiler_params=pltpu.CompilerParams(
            collective_id=0, has_side_effects=True, vmem_limit_bytes=61 * 1024 * 1024),
    )(tokens, cotangent, rw, lw)
    act, gr, gl = pl.pallas_call(
        store,
        out_shape=[jax.ShapeDtypeStruct(v.shape, v.dtype) for v in (act, gr, gl)],
        in_specs=[vmem] * 3,
        out_specs=[hbm] * 3,
        scratch_shapes=[dma((3,))],
        compiler_params=pltpu.CompilerParams(vmem_limit_bytes=1024 * 1024),
    )(act, gr, gl)
    if z.direct:
        return act, gr.reshape(z.own, z.rows, z.bs), gl.reshape(z.own, z.rows, z.bs)
    gr = gr[:, :z.own].reshape(z.mp * z.own, z.own, z.rows).transpose(1, 2, 0)
    gl = gl.reshape(z.bs, z.own, z.rows).transpose(1, 2, 0)
    return act, gr, gl


def solution(mesh):
    n_dp, n_mp = mesh.shape["dp"], mesh.shape["mp"]

    def step(tokens, right_weight, left_weight, cotangent):
        z = Sizes(n_dp, n_mp, tokens.shape[0] // n_dp, tokens.shape[1] // n_mp, right_weight.shape[1])
        return jax.shard_map(
            functools.partial(shards, z),
            mesh=mesh,
            in_specs=(P("dp", "mp"), P("mp", "dp", None), P("mp", "dp", None), P("dp", "mp")),
            out_specs=(P("dp", "mp"), P("mp", "dp", None), P("mp", "dp", None)),
            check_vma=False,
        )(tokens, right_weight, left_weight, cotangent)

    return step
```

```python
import functools

import jax
import jax.numpy as jnp
from jax import lax
from jax.experimental import pallas as pl
from jax.experimental.pallas import tpu as pltpu
from jax.sharding import PartitionSpec as P

MESH = pl.DeviceIdType.MESH
BF = jnp.bfloat16
F32 = jnp.float32
CHUNKS = 8
TAIL = (1,)


def iota(shape, dim):
    line = tuple(n if axis == dim else 1 for axis, n in enumerate(shape))
    return lax.broadcasted_iota(jnp.int32, line, dim)


def ones_where(cond):
    return jnp.where(cond, 1.0, 0.0).astype(BF)


def dot_nn(a, b):
    return lax.dot_general(a, b, (((1,), (0,)), ((), ())), preferred_element_type=F32)


def dot_nt(a, b):
    return lax.dot_general(a, b, (((1,), (1,)), ((), ())), preferred_element_type=F32)


def dot_tn(a, b):
    return lax.dot_general(a, b, (((0,), (0,)), ((), ())), preferred_element_type=F32)


def join(parts, axis=1):
    return parts[0] if len(parts) == 1 else jnp.concatenate(parts, axis=axis)


def across(index, r):
    bit = 1 << r
    return index + bit - 2 * bit * lax.rem(index // bit, 2)


class Sizes:
    def __init__(self, n_dp, n_mp, tok_rows, features, width):
        self.dp, self.mp = n_dp, n_mp
        self.tok, self.feat, self.bs = tok_rows, features, width
        self.own = features // width
        self.blocks = self.own * n_mp
        self.rows = width // n_dp
        self.orow = self.own * self.rows
        self.pad = max(self.own, 16)
        self.gs = max(1, 128 // (self.own * self.own))
        self.groups = n_mp // self.gs
        self.ng = self.gs * self.own * self.own
        self.kg = self.gs * features
        self.jg = self.ng // 128
        self.jl = self.own // self.jg
        self.nj = self.ng // self.jg
        self.rh = self.groups * self.nj
        self.fj = self.jl * width
        self.n = n_dp * n_mp
        self.direct = self.pad == self.own and self.orow % 128 == 0
        self.tc = tok_rows // CHUNKS
        self.main = CHUNKS - 1
        self.tail = []
        start = self.main * self.tc
        for part in TAIL:
            self.tail.append((self.main + len(self.tail), start, self.tc // part))
            start += self.tc // part
        self.parts = self.main + len(self.tail)
        self.n1 = CHUNKS // 2
        self.n2 = CHUNKS - self.n1
        self.split = self.direct and self.gs == 1 and self.jl == 8 and 128 % width == 0 and self.own % (256 // width) == 0
        self.rounds = n_dp.bit_length() - 1
        self.cube = n_dp == 1 << self.rounds


def kernel(z, x_hbm, cot_hbm, rw_hbm, lw_hbm, act, gr_ref, gl_ref,
           xfull, cot, rw_v, lw_v, rwt, lwt, rg, lg, p1, p2, wt, lt, gracc, glacc,
           rsend, rrecv, lsend, lrecv,
           x_recv, x_send, x_local, c_local, w_local,
           rw_send, rw_recv, lw_send, lw_recv, gr_send, gr_recv, gl_send, gl_recv, ra_send, ra_recv, met):
    d, p = lax.axis_index("dp"), lax.axis_index("mp")
    me = d * z.mp + p
    core = lax.rem(p, 2)
    partner = p + 1 - 2 * core
    chip = p // 2
    chips = z.mp // 2

    def same_core(s):
        return lax.rem(chip + s, chips) * 2 + core

    def other_core(s):
        return lax.rem(chip + s, chips) * 2 + 1 - core

    barrier = pltpu.get_barrier_semaphore()
    if z.cube:
        for s in range(1, z.mp):
            pl.semaphore_signal(barrier, inc=1, device_id=(d, lax.rem(p + s, z.mp)), device_id_type=MESH)
        for r in range(z.rounds):
            pl.semaphore_signal(barrier, inc=1, device_id=(across(d, r), p), device_id_type=MESH)
        near = z.mp - 1 + z.rounds
    else:
        @pl.loop(1, z.n)
        def _(s):
            o = lax.rem(me + s, z.n)
            pl.semaphore_signal(barrier, inc=1, device_id=(o // z.mp, lax.rem(o, z.mp)), device_id_type=MESH)
        near = z.n - 1

    def full(c):
        return c, pl.multiple_of(c * z.tc, z.tc), z.tc

    def local_x(part):
        c, start, size = part
        return pltpu.make_async_copy(x_hbm.at[pl.ds(start, size)], xfull.at[p, pl.ds(start, size)], x_local.at[c])

    def local_c(part):
        c, start, size = part
        return pltpu.make_async_copy(cot_hbm.at[pl.ds(start, size)], cot.at[pl.ds(start, size)], c_local.at[c])

    def send_own(part, kind, target):
        c, start, size = part
        return pltpu.make_async_remote_copy(
            src_ref=x_hbm.at[pl.ds(start, size)], dst_ref=xfull.at[p, pl.ds(start, size)],
            send_sem=x_send.at[kind, c], recv_sem=x_recv.at[p, c],
            device_id=(d, target), device_id_type=MESH)

    def forward(part, kind, source):
        c, start, size = part
        return pltpu.make_async_remote_copy(
            src_ref=xfull.at[source, pl.ds(start, size)], dst_ref=xfull.at[source, pl.ds(start, size)],
            send_sem=x_send.at[kind, c], recv_sem=x_recv.at[source, c],
            device_id=(d, partner), device_id_type=MESH)

    def arrived(part, source):
        c, start, size = part
        pltpu.make_async_remote_copy(
            src_ref=xfull.at[source, pl.ds(start, size)], dst_ref=xfull.at[source, pl.ds(start, size)],
            send_sem=x_send.at[0, c], recv_sem=x_recv.at[source, c],
            device_id=(d, partner), device_id_type=MESH).wait_recv()

    def each_part(step, first=0):
        @pl.loop(first, z.main)
        def _(c):
            step(full(c))
        for part in z.tail:
            step(part)

    local_r = pltpu.make_async_copy(rw_hbm, rw_v, w_local.at[0])
    local_r.start()
    local_l = pltpu.make_async_copy(lw_hbm, lw_v, w_local.at[1])
    local_l.start()

    local_r.wait()
    local_l.wait()
    shape = (z.mp * z.pad, z.bs)
    a, b = iota(shape, 0), iota(shape, 1)
    wide = ones_where((a % z.pad < z.own) & (b == (a // z.pad) * z.own + a % z.pad))
    rwt[...] = dot_nt(wide, rw_v[...]).astype(BF).reshape(z.mp, z.pad, z.orow)
    shape = (z.bs, z.bs)
    lwt[...] = dot_nt(ones_where(iota(shape, 0) == iota(shape, 1)), lw_v[...]).astype(BF)
    rg[me] = rwt[p]
    lg[d] = lwt[...]

    pl.semaphore_wait(barrier, near)

    def send_x(part):
        for s in range(1, chips):
            send_own(part, s, same_core(s)).start()
        send_own(part, 0, partner).start()

    for s in range(1, z.mp):
        q = lax.rem(p + s, z.mp)
        pltpu.make_async_remote_copy(
            src_ref=rwt.at[q], dst_ref=rg.at[me], send_sem=ra_send, recv_sem=ra_recv,
            device_id=(d, q), device_id_type=MESH).start()

    each_part(send_x)

    if z.cube:
        for r in range(z.rounds):
            pl.semaphore_signal(met.at[r], inc=1, device_id=(across(d, r), p), device_id_type=MESH)
            pl.semaphore_wait(met.at[r], 1)

    @each_part
    def _(part):
        local_x(part).start()
        local_c(part).start()

    def count(ref, sem):
        pltpu.make_async_copy(ref, ref, sem).wait()

    @pl.loop(1, z.dp)
    def _(s):
        pltpu.make_async_remote_copy(
            src_ref=lwt, dst_ref=lg.at[d], send_sem=lw_send, recv_sem=lw_recv,
            device_id=(lax.rem(d + s, z.dp), p), device_id_type=MESH).start()

    count(rg.at[pl.ds(0, z.mp - 1)], ra_recv)
    mine = rg.at[pl.ds(d * z.mp, z.mp)]

    @pl.loop(1, z.dp)
    def _(s):
        pltpu.make_async_remote_copy(
            src_ref=mine, dst_ref=mine, send_sem=rw_send, recv_sem=rw_recv,
            device_id=(lax.rem(d + s, z.dp), p), device_id_type=MESH).start()

    for dd in range(z.dp):
        shape = (z.orow, z.feat)
        a, b = iota(shape, 0), iota(shape, 1)
        source = (b // z.bs) * z.rows + (b % z.bs) - dd * z.rows
        inside = (b % z.bs) // z.rows == dd
        p1[dd] = ones_where(inside & (a == source))
        shape = (z.orow, z.blocks * z.own)
        a, b = iota(shape, 0), iota(shape, 1)
        jg = b // z.rh
        i_all = (b % z.rh) // z.jl
        j = jg * z.jl + b % z.jl
        inside = i_all // z.rows == dd
        p2[dd] = ones_where(inside & (a == j * z.rows + i_all % z.rows))
    gracc[...] = jnp.zeros_like(gracc)
    glacc[...] = jnp.zeros_like(glacc)

    count(lg.at[pl.ds(0, z.dp - 1)], lw_recv)
    left = None
    for dd in range(z.dp):
        part = dot_nn(lg[dd], p2[dd])
        left = part if left is None else left + part
    left = left.astype(BF)
    shape = (z.fj, z.bs)
    spread = ones_where(iota(shape, 0) % z.bs == iota(shape, 1))
    for jg in range(z.jg):
        piece = dot_nn(spread, left[:, jg * z.rh:(jg + 1) * z.rh])
        keep = iota((z.fj, z.rh), 0) // z.bs == iota((z.fj, z.rh), 1) % z.jl
        lt[jg] = jnp.where(keep, piece, 0.0).astype(BF)

    count(rg.at[pl.ds(0, z.n - z.mp)], rw_recv)
    right = None
    for dd in range(z.dp):
        part = dot_nn(rg[dd * z.mp:(dd + 1) * z.mp].reshape(z.mp * z.pad, z.orow), p1[dd])
        right = part if right is None else right + part
    right = right.astype(BF)
    for g in range(z.groups):
        for s in range(z.gs):
            shape = (z.ng, z.mp * z.pad)
            a, b = iota(shape, 0), iota(shape, 1)
            j = (a // z.nj) * z.jl + a % z.jl
            src = (a % z.nj) // (z.own * z.jl)
            pick = ones_where((src == s) & (b == (g * z.gs + s) * z.pad + j))
            piece = dot_nn(pick, right)
            shape = (z.ng, z.feat)
            keep = (iota(shape, 0) // z.jl) % z.own == iota(shape, 1) // z.bs
            wt[g, :, s * z.feat:(s + 1) * z.feat] = jnp.where(keep, piece, 0.0).astype(BF)

    @each_part
    def _(part):
        local_x(part).wait()
        local_c(part).wait()
        for s in range(1, chips):
            arrived(part, same_core(s))
            forward(part, chips + s, same_core(s)).start()
        arrived(part, partner)
        for s in range(1, chips):
            arrived(part, other_core(s))
        r = pl.ds(part[1], part[2])
        xs = [join([xfull[g * z.gs + s, r] for s in range(z.gs)]) for g in range(z.groups)]
        inner = [dot_nt(xs[g], wt[g]).astype(BF) for g in range(z.groups)]
        back = []
        for jg in range(z.jg):
            mixed = join([v[:, jg * z.nj:(jg + 1) * z.nj] for v in inner])
            pre = dot_nt(mixed, lt[jg])
            cdf = 0.5 * (1.0 + lax.erf(pre * 0.7071067811865476))
            slope = cdf + pre * (jnp.exp(-0.5 * pre * pre) * 0.3989422804014327)
            cols = pl.ds(jg * z.fj, z.fj)
            act[r, cols] = (pre * cdf).astype(BF)
            dpre = (cot[r, cols].astype(F32) * slope).astype(BF)
            glacc[jg] += dot_tn(dpre, mixed)
            back.append(dot_nn(dpre, lt[jg]).astype(BF))
        for g in range(z.groups):
            dinner = join([v[:, g * z.nj:(g + 1) * z.nj] for v in back])
            gracc[g] += dot_tn(dinner, xs[g])

    shape = (z.bs, z.fj)
    fold = ones_where(iota(shape, 1) % z.bs == iota(shape, 0))
    lefts = []
    for jg in range(z.jg):
        keep = iota((z.fj, z.rh), 0) // z.bs == iota((z.fj, z.rh), 1) % z.jl
        lefts.append(dot_nn(fold, jnp.where(keep, glacc[jg], 0.0).astype(BF)).astype(BF))
    left = join(lefts)
    for dd in range(z.dp):
        lsend[dd] = dot_nt(left, p2[dd]).astype(BF)

    @pl.loop(1, z.dp)
    def _(s):
        o = lax.rem(d + s, z.dp)
        pltpu.make_async_remote_copy(
            src_ref=lsend.at[o], dst_ref=lrecv.at[d], send_sem=gl_send, recv_sem=gl_recv,
            device_id=(o, p), device_id_type=MESH).start()

    pieces = []
    for g in range(z.groups):
        for s in range(z.gs):
            shape = (z.pad, z.ng)
            a, b = iota(shape, 0), iota(shape, 1)
            j = (b // z.nj) * z.jl + b % z.jl
            src = (b % z.nj) // (z.own * z.jl)
            pick = ones_where((src == s) & (a == j))
            shape = (z.ng, z.feat)
            keep = (iota(shape, 0) // z.jl) % z.own == iota(shape, 1) // z.bs
            piece = jnp.where(keep, gracc[g, :, s * z.feat:(s + 1) * z.feat], 0.0).astype(BF)
            pieces.append(dot_nn(pick, piece).astype(BF))
    pieces = join(pieces, axis=0)
    for dd in range(z.dp):
        owned = dot_nt(pieces, p1[dd]).astype(BF)
        rsend[dd * z.mp:(dd + 1) * z.mp] = owned.reshape(z.mp, z.pad, z.orow)

    @pl.loop(1, z.n)
    def _(s):
        o = lax.rem(me + s, z.n)
        pltpu.make_async_remote_copy(
            src_ref=rsend.at[o], dst_ref=rrecv.at[me], send_sem=gr_send, recv_sem=gr_recv,
            device_id=(o // z.mp, lax.rem(o, z.mp)), device_id_type=MESH).start()

    lrecv[d] = lsend[d]
    rrecv[me] = rsend[me]

    @each_part
    def _(part):
        for s in range(1, chips):
            send_own(part, s, same_core(s)).wait_send()
            forward(part, chips + s, same_core(s)).wait_send()
        send_own(part, 0, partner).wait_send()

    count(rg.at[pl.ds(0, z.mp - 1)], ra_send)
    count(rg.at[pl.ds(0, z.n - z.mp)], rw_send)
    count(lg.at[pl.ds(0, z.dp - 1)], lw_send)

    count(lrecv.at[pl.ds(0, z.dp - 1)], gl_recv)
    total = lrecv[0].astype(F32)
    for dd in range(1, z.dp):
        total = total + lrecv[dd].astype(F32)
    gl_ref[...] = total.T if z.direct else total
    count(rrecv.at[pl.ds(0, z.n - 1)], gr_recv)
    total = rrecv[0:z.mp].astype(F32)
    for dd in range(1, z.dp):
        total = total + rrecv[dd * z.mp:(dd + 1) * z.mp].astype(F32)
    gr_ref[...] = total.reshape(z.blocks, z.orow).T if z.direct else total
    count(lsend.at[pl.ds(0, z.dp - 1)], gl_send)
    count(rsend.at[pl.ds(0, z.n - 1)], gr_send)


def split_kernel(z, x_hbm, cot_hbm, rw_hbm, lw_hbm, act, gr_ref, gl_ref,
                 xfull, x2, cot, rw_v, lw_v, rwt, lwt, rg, rg2, lg, p1, p2, wt, wt2, lt, gracc, glacc,
                 isend, irecv, dsend, drecv, fsend, frecv, rsend, rrecv, lsend, lrecv,
                 x_recv, x_send, x_local, c_local, w_local, i_send, i_recv, d_send, d_recv,
                 f_send, f_recv, gr_send, gr_recv,
                 rw_send, rw_recv, lw_send, lw_recv, gl_send, gl_recv, ra_send, ra_recv, rb_send, rb_recv, met):
    d, p = lax.axis_index("dp"), lax.axis_index("mp")
    me = d * z.mp + p
    core = lax.rem(p, 2)
    partner = p + 1 - 2 * core
    chip = p // 2
    chips = z.mp // 2
    n1, n2, tc = z.n1, z.n2, z.tc
    first = n1 * tc

    def same_core(s):
        return lax.rem(chip + s, chips) * 2 + core

    def other_core(s):
        return lax.rem(chip + s, chips) * 2 + 1 - core

    barrier = pltpu.get_barrier_semaphore()
    if z.cube:
        for s in range(1, z.mp):
            pl.semaphore_signal(barrier, inc=1, device_id=(d, lax.rem(p + s, z.mp)), device_id_type=MESH)
        for r in range(z.rounds):
            pl.semaphore_signal(barrier, inc=1, device_id=(across(d, r), p), device_id_type=MESH)
        near = z.mp - 1 + z.rounds
    else:
        @pl.loop(1, z.n)
        def _(s):
            o = lax.rem(me + s, z.n)
            pl.semaphore_signal(barrier, inc=1, device_id=(o // z.mp, lax.rem(o, z.mp)), device_id_type=MESH)
        near = z.n - 1

    def rows(c):
        return pl.ds(pl.multiple_of(c * tc, tc), tc)

    def later(c):
        return pl.ds(pl.multiple_of(first + c * tc, tc), tc)

    def local_x(c):
        return pltpu.make_async_copy(x_hbm.at[rows(c)], xfull.at[p, rows(c)], x_local.at[c])

    def local_x2(c):
        return pltpu.make_async_copy(x_hbm.at[later(c)], x2.at[rows(c)], x_local.at[n1 + c])

    def local_c(c):
        return pltpu.make_async_copy(cot_hbm.at[rows(c)], cot.at[rows(c)], c_local.at[c])

    def send_own(c, kind, target):
        return pltpu.make_async_remote_copy(
            src_ref=x_hbm.at[rows(c)], dst_ref=xfull.at[p, rows(c)],
            send_sem=x_send.at[kind, c], recv_sem=x_recv.at[p, c],
            device_id=(d, target), device_id_type=MESH)

    def forward(c, kind, source):
        return pltpu.make_async_remote_copy(
            src_ref=xfull.at[source, rows(c)], dst_ref=xfull.at[source, rows(c)],
            send_sem=x_send.at[kind, c], recv_sem=x_recv.at[source, c],
            device_id=(d, partner), device_id_type=MESH)

    def arrived(c, source):
        forward(c, 0, source).wait_recv()

    def each_mp(send):
        for s in range(1, chips):
            send(same_core(s))
            send(other_core(s))
        send(partner)

    def send_inner(c, q):
        pltpu.make_async_remote_copy(
            src_ref=isend.at[q, rows(c)], dst_ref=irecv.at[p, rows(c)],
            send_sem=i_send.at[c], recv_sem=i_recv.at[c],
            device_id=(d, q), device_id_type=MESH).start()

    def send_dinner(c, jg, q):
        pltpu.make_async_remote_copy(
            src_ref=dsend.at[jg, q, rows(c)], dst_ref=drecv.at[jg, p, rows(c)],
            send_sem=d_send.at[jg, c], recv_sem=d_recv.at[jg, c],
            device_id=(d, q), device_id_type=MESH).start()

    def send_first(q):
        pltpu.make_async_remote_copy(
            src_ref=fsend.at[q], dst_ref=frecv.at[p], send_sem=f_send, recv_sem=f_recv,
            device_id=(d, q), device_id_type=MESH).start()

    def count(ref, sem):
        pltpu.make_async_copy(ref, ref, sem).wait()

    def others(ref):
        return ref.at[pl.ds(0, z.mp - 1)]

    local_r = pltpu.make_async_copy(rw_hbm, rw_v, w_local.at[0])
    local_r.start()
    local_l = pltpu.make_async_copy(lw_hbm, lw_v, w_local.at[1])
    local_l.start()
    local_r.wait()
    local_l.wait()
    shape = (z.mp * z.pad, z.bs)
    a, b = iota(shape, 0), iota(shape, 1)
    wide = ones_where((a % z.pad < z.own) & (b == (a // z.pad) * z.own + a % z.pad))
    rwt[...] = dot_nt(wide, rw_v[...]).astype(BF).reshape(z.mp, z.pad, z.orow)
    shape = (z.bs, z.bs)
    lwt[...] = dot_nt(ones_where(iota(shape, 0) == iota(shape, 1)), lw_v[...]).astype(BF)
    rg[me] = rwt[p]
    rg2[d] = rwt[...]
    lg[d] = lwt[...]
    pl.semaphore_wait(barrier, near)

    for s in range(1, z.mp):
        q = lax.rem(p + s, z.mp)
        pltpu.make_async_remote_copy(
            src_ref=rwt.at[q], dst_ref=rg.at[me], send_sem=ra_send, recv_sem=ra_recv,
            device_id=(d, q), device_id_type=MESH).start()

    @pl.loop(0, n1)
    def _(c):
        for s in range(1, chips):
            send_own(c, s, same_core(s)).start()
        send_own(c, 0, partner).start()

    if z.cube:
        for r in range(z.rounds):
            pl.semaphore_signal(met.at[r], inc=1, device_id=(across(d, r), p), device_id_type=MESH)
            pl.semaphore_wait(met.at[r], 1)

    @pl.loop(0, n1)
    def _(c):
        local_x(c).start()
        local_c(c).start()

    @pl.loop(0, n2)
    def _(c):
        local_x2(c).start()
        local_c(n1 + c).start()

    @pl.loop(1, z.dp)
    def _(s):
        pltpu.make_async_remote_copy(
            src_ref=lwt, dst_ref=lg.at[d], send_sem=lw_send, recv_sem=lw_recv,
            device_id=(lax.rem(d + s, z.dp), p), device_id_type=MESH).start()

    count(others(rg), ra_recv)
    mine = rg.at[pl.ds(d * z.mp, z.mp)]

    @pl.loop(1, z.dp)
    def _(s):
        pltpu.make_async_remote_copy(
            src_ref=mine, dst_ref=mine, send_sem=rw_send, recv_sem=rw_recv,
            device_id=(lax.rem(d + s, z.dp), p), device_id_type=MESH).start()

    @pl.loop(1, z.dp)
    def _(s):
        pltpu.make_async_remote_copy(
            src_ref=rwt, dst_ref=rg2.at[d], send_sem=rb_send, recv_sem=rb_recv,
            device_id=(lax.rem(d + s, z.dp), p), device_id_type=MESH).start()

    for dd in range(z.dp):
        shape = (z.orow, z.feat)
        a, b = iota(shape, 0), iota(shape, 1)
        source = (b // z.bs) * z.rows + (b % z.bs) - dd * z.rows
        inside = (b % z.bs) // z.rows == dd
        p1[dd] = ones_where(inside & (a == source))
        shape = (z.orow, z.blocks * z.own)
        a, b = iota(shape, 0), iota(shape, 1)
        jg = b // z.rh
        i_all = (b % z.rh) // z.jl
        j = jg * z.jl + b % z.jl
        inside = i_all // z.rows == dd
        p2[dd] = ones_where(inside & (a == j * z.rows + i_all % z.rows))
    gracc[...] = jnp.zeros_like(gracc)
    glacc[...] = jnp.zeros_like(glacc)

    count(lg.at[pl.ds(0, z.dp - 1)], lw_recv)
    left = None
    for dd in range(z.dp):
        part = dot_nn(lg[dd], p2[dd])
        left = part if left is None else left + part
    left = left.astype(BF)
    shape = (z.fj, z.bs)
    spread = ones_where(iota(shape, 0) % z.bs == iota(shape, 1))
    for jg in range(z.jg):
        piece = dot_nn(spread, left[:, jg * z.rh:(jg + 1) * z.rh])
        keep = iota((z.fj, z.rh), 0) // z.bs == iota((z.fj, z.rh), 1) % z.jl
        lt[jg] = jnp.where(keep, piece, 0.0).astype(BF)

    def expand(blocks, target):
        right = None
        for dd in range(z.dp):
            part = dot_nn(blocks(dd).reshape(z.mp * z.pad, z.orow), p1[dd])
            right = part if right is None else right + part
        right = right.astype(BF)
        for g in range(z.mp):
            shape = (z.ng, z.mp * z.pad)
            a, b = iota(shape, 0), iota(shape, 1)
            pick = ones_where(b == g * z.pad + (a // z.nj) * z.jl + a % z.jl)
            piece = dot_nn(pick, right)
            shape = (z.ng, z.feat)
            keep = (iota(shape, 0) // z.jl) % z.own == iota(shape, 1) // z.bs
            target[g] = jnp.where(keep, piece, 0.0).astype(BF)

    count(rg.at[pl.ds(0, z.n - z.mp)], rw_recv)
    expand(lambda dd: rg[dd * z.mp:(dd + 1) * z.mp], wt)
    count(rg2.at[pl.ds(0, z.dp - 1)], rb_recv)
    expand(lambda dd: rg2[dd], wt2)

    def layer(inner, r):
        back = []
        for jg in range(z.jg):
            mixed = join([v[:, jg * z.nj:(jg + 1) * z.nj] for v in inner])
            pre = dot_nt(mixed, lt[jg])
            cdf = 0.5 * (1.0 + lax.erf(pre * 0.7071067811865476))
            slope = cdf + pre * (jnp.exp(-0.5 * pre * pre) * 0.3989422804014327)
            cols = pl.ds(jg * z.fj, z.fj)
            act[r, cols] = (pre * cdf).astype(BF)
            dpre = (cot[r, cols].astype(F32) * slope).astype(BF)
            glacc[jg] += dot_tn(dpre, mixed)
            back.append(dot_nn(dpre, lt[jg]).astype(BF))
        return back

    @pl.loop(0, n1)
    def _(c):
        local_x(c).wait()
        local_c(c).wait()
        for s in range(1, chips):
            arrived(c, same_core(s))
            forward(c, chips + s, same_core(s)).start()
        arrived(c, partner)
        for s in range(1, chips):
            arrived(c, other_core(s))
        r = rows(c)
        xs = [xfull[g, r] for g in range(z.mp)]
        back = layer([dot_nt(xs[g], wt[g]).astype(BF) for g in range(z.mp)], r)
        for g in range(z.mp):
            dinner = join([v[:, g * z.nj:(g + 1) * z.nj] for v in back])
            gracc[g] += dot_tn(dinner, xs[g])

        @pl.loop(c * n2 // n1, (c + 1) * n2 // n1)
        def _(e):
            local_x2(e).wait()
            own = x2[rows(e)]
            for q in range(z.mp):
                isend[q, rows(e)] = dot_nt(own, wt2[q]).astype(BF)
            each_mp(functools.partial(send_inner, e))
            irecv[p, rows(e)] = isend[p, rows(e)]

    per = 128 // z.bs
    lane = iota((z.jl, 128), 1) // z.bs

    def diagonal(tile):
        parts = []
        for v in range(z.own // per):
            piece = tile(v * per, v)
            for w in range(1, per):
                piece = jnp.where(lane == w, tile(v * per + w, v), piece)
            parts.append(piece)
        return join(parts)

    for g in range(z.mp):
        halves = []
        for jg in range(z.jg):
            halves.append(diagonal(lambda i, v: gracc[
                g, jg * z.nj + i * z.jl:jg * z.nj + (i + 1) * z.jl, v * 128:(v + 1) * 128]))
        fsend[g] = join(halves, axis=0).astype(BF)
    each_mp(send_first)
    frecv[p] = fsend[p]

    @pl.loop(0, n2)
    def _(c):
        local_c(n1 + c).wait()
        r = rows(c)
        count(irecv.at[pl.ds(0, z.mp - 1), r], i_recv.at[c])
        back = layer([irecv[g, r] for g in range(z.mp)], later(c))
        for jg in range(z.jg):
            for g in range(z.mp):
                dsend[jg, g, r] = back[jg][:, g * z.nj:(g + 1) * z.nj]
            drecv[jg, p, r] = dsend[jg, p, r]
        each_mp(functools.partial(send_dinner, c, 0))

    for jg in range(1, z.jg):
        @pl.loop(0, n2)
        def _(c):
            each_mp(functools.partial(send_dinner, c, jg))

    shape = (z.bs, z.fj)
    fold = ones_where(iota(shape, 1) % z.bs == iota(shape, 0))
    lefts = []
    for jg in range(z.jg):
        keep = iota((z.fj, z.rh), 0) // z.bs == iota((z.fj, z.rh), 1) % z.jl
        lefts.append(dot_nn(fold, jnp.where(keep, glacc[jg], 0.0).astype(BF)).astype(BF))
    left = join(lefts)
    for dd in range(z.dp):
        lsend[dd] = dot_nt(left, p2[dd]).astype(BF)

    @pl.loop(1, z.dp)
    def _(s):
        o = lax.rem(d + s, z.dp)
        pltpu.make_async_remote_copy(
            src_ref=lsend.at[o], dst_ref=lrecv.at[d], send_sem=gl_send, recv_sem=gl_recv,
            device_id=(o, p), device_id_type=MESH).start()
    lrecv[d] = lsend[d]

    quad = 256 // z.bs

    def piece_of(jg, lo, hi):
        turned = [drecv[jg, q, lo * tc:hi * tc].T for q in range(z.mp)]
        parts = []
        for a in range(z.own // quad):
            m = quad * z.jl
            lhs = join([t[a * m:(a + 1) * m] for t in turned], axis=0)
            full = dot_nn(lhs, x2[lo * tc:hi * tc, a * 256:(a + 1) * 256])
            blocks = []
            for q in range(z.mp):
                tiles = []
                for v in range(quad // per):
                    base = q * m + v * per * z.jl
                    piece = full[base:base + z.jl, v * 128:(v + 1) * 128]
                    for w in range(1, per):
                        base += z.jl
                        piece = jnp.where(lane == w, full[base:base + z.jl, v * 128:(v + 1) * 128], piece)
                    tiles.append(piece)
                blocks.append(join(tiles))
            parts.append(join(blocks, axis=0))
        return join(parts)

    count(others(frecv), f_recv)
    early = frecv[...].astype(F32)
    for jg in range(z.jg):
        total = join([early[q, jg * z.jl:(jg + 1) * z.jl] for q in range(z.mp)], axis=0)
        cuts = (0, n2) if jg < z.jg - 1 or n2 < 2 else (0, n2 - 1, n2)
        for lo, hi in zip(cuts[:-1], cuts[1:]):
            for c in range(lo, hi):
                count(drecv.at[jg, pl.ds(0, z.mp - 1), pl.ds(c * tc, tc)], d_recv.at[jg, c])
            total = total + piece_of(jg, lo, hi)
        total = total.astype(BF)
        for dd in range(z.dp):
            rsend[jg, dd] = dot_nt(total, p1[dd]).astype(BF)

        @pl.loop(1, z.dp)
        def _(s):
            o = lax.rem(d + s, z.dp)
            pltpu.make_async_remote_copy(
                src_ref=rsend.at[jg, o], dst_ref=rrecv.at[jg, d],
                send_sem=gr_send.at[jg], recv_sem=gr_recv.at[jg],
                device_id=(o, p), device_id_type=MESH).start()
        rrecv[jg, d] = rsend[jg, d]

    @pl.loop(0, n1)
    def _(c):
        for s in range(1, chips):
            send_own(c, s, same_core(s)).wait_send()
            forward(c, chips + s, same_core(s)).wait_send()
        send_own(c, 0, partner).wait_send()

    @pl.loop(0, n2)
    def _(c):
        count(isend.at[pl.ds(0, z.mp - 1), rows(c)], i_send.at[c])
        for jg in range(z.jg):
            count(dsend.at[jg, pl.ds(0, z.mp - 1), rows(c)], d_send.at[jg, c])

    count(others(rg), ra_send)
    count(others(fsend), f_send)
    count(rg.at[pl.ds(0, z.n - z.mp)], rw_send)
    count(rg2.at[pl.ds(0, z.dp - 1)], rb_send)
    count(lg.at[pl.ds(0, z.dp - 1)], lw_send)

    count(lrecv.at[pl.ds(0, z.dp - 1)], gl_recv)
    total = lrecv[0].astype(F32)
    for dd in range(1, z.dp):
        total = total + lrecv[dd].astype(F32)
    gl_ref[...] = total.T
    totals = []
    for jg in range(z.jg):
        count(rrecv.at[jg, pl.ds(0, z.dp - 1)], gr_recv.at[jg])
        total = rrecv[jg, 0].astype(F32)
        for dd in range(1, z.dp):
            total = total + rrecv[jg, dd].astype(F32)
        totals.append(total)
    total = join([t[q * z.jl:(q + 1) * z.jl] for q in range(z.mp) for t in totals], axis=0)
    gr_ref[...] = total.T
    count(lsend.at[pl.ds(0, z.dp - 1)], gl_send)
    for jg in range(z.jg):
        count(rsend.at[jg, pl.ds(0, z.dp - 1)], gr_send.at[jg])


def split_scratch(z):
    dma = pltpu.SemaphoreType.DMA
    return [
        pltpu.VMEM((z.mp, z.n1 * z.tc, z.feat), BF),
        pltpu.VMEM((z.n2 * z.tc, z.feat), BF),
        pltpu.VMEM((z.tok, z.feat), BF),
        pltpu.VMEM((z.orow, z.bs), BF),
        pltpu.VMEM((z.orow, z.bs), BF),
        pltpu.VMEM((z.mp, z.pad, z.orow), BF),
        pltpu.VMEM((z.bs, z.orow), BF),
        pltpu.VMEM((z.n, z.pad, z.orow), BF),
        pltpu.VMEM((z.dp, z.mp, z.pad, z.orow), BF),
        pltpu.VMEM((z.dp, z.bs, z.orow), BF),
        pltpu.VMEM((z.dp, z.orow, z.feat), BF),
        pltpu.VMEM((z.dp, z.orow, z.blocks * z.own), BF),
        pltpu.VMEM((z.mp, z.ng, z.feat), BF),
        pltpu.VMEM((z.mp, z.ng, z.feat), BF),
        pltpu.VMEM((z.jg, z.fj, z.rh), BF),
        pltpu.VMEM((z.mp, z.ng, z.feat), F32),
        pltpu.VMEM((z.jg, z.fj, z.rh), F32),
        pltpu.VMEM((z.mp, z.n2 * z.tc, z.ng), BF),
        pltpu.VMEM((z.mp, z.n2 * z.tc, z.ng), BF),
        pltpu.VMEM((z.jg, z.mp, z.n2 * z.tc, z.nj), BF),
        pltpu.VMEM((z.jg, z.mp, z.n2 * z.tc, z.nj), BF),
        pltpu.VMEM((z.mp, z.own, z.feat), BF),
        pltpu.VMEM((z.mp, z.own, z.feat), BF),
        pltpu.VMEM((z.jg, z.dp, z.mp * z.jl, z.orow), BF),
        pltpu.VMEM((z.jg, z.dp, z.mp * z.jl, z.orow), BF),
        pltpu.VMEM((z.dp, z.bs, z.orow), BF),
        pltpu.VMEM((z.dp, z.bs, z.orow), BF),
        dma((z.mp, z.n1)),
        dma((z.mp, z.n1)),
        dma((CHUNKS,)),
        dma((CHUNKS,)),
        dma((2,)),
        dma((z.n2,)),
        dma((z.n2,)),
        dma((z.jg, z.n2)),
        dma((z.jg, z.n2)),
        dma, dma,
        dma((z.jg,)),
        dma((z.jg,)),
        dma, dma, dma, dma, dma, dma, dma, dma, dma, dma,
        pltpu.SemaphoreType.REGULAR((max(1, z.rounds),)),
    ]


def store(*refs):
    sems = refs[6]
    copies = [pltpu.make_async_copy(refs[k], refs[k + 3], sems.at[k]) for k in range(3)]
    for copy in copies:
        copy.start()
    for copy in copies:
        copy.wait()


def shards(z, tokens, right_weight, left_weight, cotangent):
    rw = right_weight.reshape(z.orow, z.bs)
    lw = left_weight.reshape(z.orow, z.bs)
    hbm = pl.BlockSpec(memory_space=pltpu.HBM)
    vmem = pl.BlockSpec(memory_space=pltpu.VMEM)
    dma = pltpu.SemaphoreType.DMA
    act, gr, gl = pl.pallas_call(
        functools.partial(split_kernel if z.split else kernel, z),
        out_shape=(
            pltpu.VMEM((z.tok, z.feat), BF),
            pltpu.VMEM((z.orow, z.bs) if z.direct else (z.mp, z.pad, z.orow), F32),
            pltpu.VMEM((z.orow, z.bs) if z.direct else (z.bs, z.orow), F32),
        ),
        in_specs=[hbm] * 4,
        out_specs=(vmem, vmem, vmem),
        scratch_shapes=split_scratch(z) if z.split else [
            pltpu.VMEM((z.mp, z.tok, z.feat), BF),
            pltpu.VMEM((z.tok, z.feat), BF),
            pltpu.VMEM((z.orow, z.bs), BF),
            pltpu.VMEM((z.orow, z.bs), BF),
            pltpu.VMEM((z.mp, z.pad, z.orow), BF),
            pltpu.VMEM((z.bs, z.orow), BF),
            pltpu.VMEM((z.n, z.pad, z.orow), BF),
            pltpu.VMEM((z.dp, z.bs, z.orow), BF),
            pltpu.VMEM((z.dp, z.orow, z.feat), BF),
            pltpu.VMEM((z.dp, z.orow, z.blocks * z.own), BF),
            pltpu.VMEM((z.groups, z.ng, z.kg), BF),
            pltpu.VMEM((z.jg, z.fj, z.rh), BF),
            pltpu.VMEM((z.groups, z.ng, z.kg), F32),
            pltpu.VMEM((z.jg, z.fj, z.rh), F32),
            pltpu.VMEM((z.n, z.pad, z.orow), BF),
            pltpu.VMEM((z.n, z.pad, z.orow), BF),
            pltpu.VMEM((z.dp, z.bs, z.orow), BF),
            pltpu.VMEM((z.dp, z.bs, z.orow), BF),
            dma((z.mp, z.parts)),
            dma((z.mp, z.parts)),
            dma((z.parts,)),
            dma((z.parts,)),
            dma((2,)),
            dma, dma, dma, dma, dma, dma, dma, dma, dma, dma,
            pltpu.SemaphoreType.REGULAR((max(1, z.rounds),)),
        ],
        compiler_params=pltpu.CompilerParams(
            collective_id=0, has_side_effects=True, vmem_limit_bytes=61 * 1024 * 1024),
    )(tokens, cotangent, rw, lw)
    act, gr, gl = pl.pallas_call(
        store,
        out_shape=[jax.ShapeDtypeStruct(v.shape, v.dtype) for v in (act, gr, gl)],
        in_specs=[vmem] * 3,
        out_specs=[hbm] * 3,
        scratch_shapes=[dma((3,))],
        compiler_params=pltpu.CompilerParams(vmem_limit_bytes=1024 * 1024),
    )(act, gr, gl)
    if z.direct:
        return act, gr.reshape(z.own, z.rows, z.bs), gl.reshape(z.own, z.rows, z.bs)
    gr = gr[:, :z.own].reshape(z.mp * z.own, z.own, z.rows).transpose(1, 2, 0)
    gl = gl.reshape(z.bs, z.own, z.rows).transpose(1, 2, 0)
    return act, gr, gl


def solution(mesh):
    n_dp, n_mp = mesh.shape["dp"], mesh.shape["mp"]

    def step(tokens, right_weight, left_weight, cotangent):
        z = Sizes(n_dp, n_mp, tokens.shape[0] // n_dp, tokens.shape[1] // n_mp, right_weight.shape[1])
        return jax.shard_map(
            functools.partial(shards, z),
            mesh=mesh,
            in_specs=(P("dp", "mp"), P("mp", "dp", None), P("mp", "dp", None), P("dp", "mp")),
            out_specs=(P("dp", "mp"), P("mp", "dp", None), P("mp", "dp", None)),
            check_vma=False,
        )(tokens, right_weight, left_weight, cotangent)

    return step
```

```python
import functools

import jax
import jax.numpy as jnp
from jax import lax
from jax.experimental import pallas as pl
from jax.experimental.pallas import tpu as pltpu
from jax.sharding import PartitionSpec as P

MESH = pl.DeviceIdType.MESH
BF = jnp.bfloat16
F32 = jnp.float32
CHUNKS = 8
TAIL = (1,)


def iota(shape, dim):
    line = tuple(n if axis == dim else 1 for axis, n in enumerate(shape))
    return lax.broadcasted_iota(jnp.int32, line, dim)


def ones_where(cond):
    return jnp.where(cond, 1.0, 0.0).astype(BF)


def dot_nn(a, b):
    return lax.dot_general(a, b, (((1,), (0,)), ((), ())), preferred_element_type=F32)


def dot_nt(a, b):
    return lax.dot_general(a, b, (((1,), (1,)), ((), ())), preferred_element_type=F32)


def dot_tn(a, b):
    return lax.dot_general(a, b, (((0,), (0,)), ((), ())), preferred_element_type=F32)


def join(parts, axis=1):
    return parts[0] if len(parts) == 1 else jnp.concatenate(parts, axis=axis)


def across(index, r):
    bit = 1 << r
    return index + bit - 2 * bit * lax.rem(index // bit, 2)


class Sizes:
    def __init__(self, n_dp, n_mp, tok_rows, features, width):
        self.dp, self.mp = n_dp, n_mp
        self.tok, self.feat, self.bs = tok_rows, features, width
        self.own = features // width
        self.blocks = self.own * n_mp
        self.rows = width // n_dp
        self.orow = self.own * self.rows
        self.pad = max(self.own, 16)
        self.gs = max(1, 128 // (self.own * self.own))
        self.groups = n_mp // self.gs
        self.ng = self.gs * self.own * self.own
        self.kg = self.gs * features
        self.jg = self.ng // 128
        self.jl = self.own // self.jg
        self.nj = self.ng // self.jg
        self.rh = self.groups * self.nj
        self.fj = self.jl * width
        self.n = n_dp * n_mp
        self.direct = self.pad == self.own and self.orow % 128 == 0
        self.tc = tok_rows // CHUNKS
        self.main = CHUNKS - 1
        self.tail = []
        start = self.main * self.tc
        for part in TAIL:
            self.tail.append((self.main + len(self.tail), start, self.tc // part))
            start += self.tc // part
        self.parts = self.main + len(self.tail)
        self.n1 = CHUNKS // 2
        self.n2 = CHUNKS - self.n1
        self.early = min(2, self.n1)
        self.quad = 256 // width
        self.quads = self.own // max(1, self.quad)
        self.unit = self.quad * self.rows
        self.slots = 128 // self.unit
        self.units = self.jg * (n_mp // 2)
        self.split = self.gs == 1 and self.jl == 8 and self.rows == 8 and self.orow == 128 and width == 64 and n_mp == 4
        self.rounds = n_dp.bit_length() - 1
        self.cube = n_dp == 1 << self.rounds


def kernel(z, x_hbm, cot_hbm, rw_hbm, lw_hbm, act, gr_ref, gl_ref,
           xfull, cot, rw_v, lw_v, rwt, lwt, rg, lg, p1, p2, wt, lt, gracc, glacc,
           rsend, rrecv, lsend, lrecv,
           x_recv, x_send, x_local, c_local, w_local,
           rw_send, rw_recv, lw_send, lw_recv, gr_send, gr_recv, gl_send, gl_recv, ra_send, ra_recv, met):
    d, p = lax.axis_index("dp"), lax.axis_index("mp")
    me = d * z.mp + p
    core = lax.rem(p, 2)
    partner = p + 1 - 2 * core
    chip = p // 2
    chips = z.mp // 2

    def same_core(s):
        return lax.rem(chip + s, chips) * 2 + core

    def other_core(s):
        return lax.rem(chip + s, chips) * 2 + 1 - core

    barrier = pltpu.get_barrier_semaphore()
    if z.cube:
        for s in range(1, z.mp):
            pl.semaphore_signal(barrier, inc=1, device_id=(d, lax.rem(p + s, z.mp)), device_id_type=MESH)
        for r in range(z.rounds):
            pl.semaphore_signal(barrier, inc=1, device_id=(across(d, r), p), device_id_type=MESH)
        near = z.mp - 1 + z.rounds
    else:
        @pl.loop(1, z.n)
        def _(s):
            o = lax.rem(me + s, z.n)
            pl.semaphore_signal(barrier, inc=1, device_id=(o // z.mp, lax.rem(o, z.mp)), device_id_type=MESH)
        near = z.n - 1

    def full(c):
        return c, pl.multiple_of(c * z.tc, z.tc), z.tc

    def local_x(part):
        c, start, size = part
        return pltpu.make_async_copy(x_hbm.at[pl.ds(start, size)], xfull.at[p, pl.ds(start, size)], x_local.at[c])

    def local_c(part):
        c, start, size = part
        return pltpu.make_async_copy(cot_hbm.at[pl.ds(start, size)], cot.at[pl.ds(start, size)], c_local.at[c])

    def send_own(part, kind, target):
        c, start, size = part
        return pltpu.make_async_remote_copy(
            src_ref=x_hbm.at[pl.ds(start, size)], dst_ref=xfull.at[p, pl.ds(start, size)],
            send_sem=x_send.at[kind, c], recv_sem=x_recv.at[p, c],
            device_id=(d, target), device_id_type=MESH)

    def forward(part, kind, source):
        c, start, size = part
        return pltpu.make_async_remote_copy(
            src_ref=xfull.at[source, pl.ds(start, size)], dst_ref=xfull.at[source, pl.ds(start, size)],
            send_sem=x_send.at[kind, c], recv_sem=x_recv.at[source, c],
            device_id=(d, partner), device_id_type=MESH)

    def arrived(part, source):
        c, start, size = part
        pltpu.make_async_remote_copy(
            src_ref=xfull.at[source, pl.ds(start, size)], dst_ref=xfull.at[source, pl.ds(start, size)],
            send_sem=x_send.at[0, c], recv_sem=x_recv.at[source, c],
            device_id=(d, partner), device_id_type=MESH).wait_recv()

    def each_part(step, first=0):
        @pl.loop(first, z.main)
        def _(c):
            step(full(c))
        for part in z.tail:
            step(part)

    local_r = pltpu.make_async_copy(rw_hbm, rw_v, w_local.at[0])
    local_r.start()
    local_l = pltpu.make_async_copy(lw_hbm, lw_v, w_local.at[1])
    local_l.start()

    local_r.wait()
    local_l.wait()
    shape = (z.mp * z.pad, z.bs)
    a, b = iota(shape, 0), iota(shape, 1)
    wide = ones_where((a % z.pad < z.own) & (b == (a // z.pad) * z.own + a % z.pad))
    rwt[...] = dot_nt(wide, rw_v[...]).astype(BF).reshape(z.mp, z.pad, z.orow)
    shape = (z.bs, z.bs)
    lwt[...] = dot_nt(ones_where(iota(shape, 0) == iota(shape, 1)), lw_v[...]).astype(BF)
    rg[me] = rwt[p]
    lg[d] = lwt[...]

    pl.semaphore_wait(barrier, near)

    def send_x(part):
        for s in range(1, chips):
            send_own(part, s, same_core(s)).start()
        send_own(part, 0, partner).start()

    for s in range(1, z.mp):
        q = lax.rem(p + s, z.mp)
        pltpu.make_async_remote_copy(
            src_ref=rwt.at[q], dst_ref=rg.at[me], send_sem=ra_send, recv_sem=ra_recv,
            device_id=(d, q), device_id_type=MESH).start()

    each_part(send_x)

    if z.cube:
        for r in range(z.rounds):
            pl.semaphore_signal(met.at[r], inc=1, device_id=(across(d, r), p), device_id_type=MESH)
            pl.semaphore_wait(met.at[r], 1)

    @each_part
    def _(part):
        local_x(part).start()
        local_c(part).start()

    def count(ref, sem):
        pltpu.make_async_copy(ref, ref, sem).wait()

    @pl.loop(1, z.dp)
    def _(s):
        pltpu.make_async_remote_copy(
            src_ref=lwt, dst_ref=lg.at[d], send_sem=lw_send, recv_sem=lw_recv,
            device_id=(lax.rem(d + s, z.dp), p), device_id_type=MESH).start()

    count(rg.at[pl.ds(0, z.mp - 1)], ra_recv)
    mine = rg.at[pl.ds(d * z.mp, z.mp)]

    @pl.loop(1, z.dp)
    def _(s):
        pltpu.make_async_remote_copy(
            src_ref=mine, dst_ref=mine, send_sem=rw_send, recv_sem=rw_recv,
            device_id=(lax.rem(d + s, z.dp), p), device_id_type=MESH).start()

    for dd in range(z.dp):
        shape = (z.orow, z.feat)
        a, b = iota(shape, 0), iota(shape, 1)
        source = (b // z.bs) * z.rows + (b % z.bs) - dd * z.rows
        inside = (b % z.bs) // z.rows == dd
        p1[dd] = ones_where(inside & (a == source))
        shape = (z.orow, z.blocks * z.own)
        a, b = iota(shape, 0), iota(shape, 1)
        jg = b // z.rh
        i_all = (b % z.rh) // z.jl
        j = jg * z.jl + b % z.jl
        inside = i_all // z.rows == dd
        p2[dd] = ones_where(inside & (a == j * z.rows + i_all % z.rows))
    gracc[...] = jnp.zeros_like(gracc)
    glacc[...] = jnp.zeros_like(glacc)

    count(lg.at[pl.ds(0, z.dp - 1)], lw_recv)
    left = None
    for dd in range(z.dp):
        part = dot_nn(lg[dd], p2[dd])
        left = part if left is None else left + part
    left = left.astype(BF)
    shape = (z.fj, z.bs)
    spread = ones_where(iota(shape, 0) % z.bs == iota(shape, 1))
    for jg in range(z.jg):
        piece = dot_nn(spread, left[:, jg * z.rh:(jg + 1) * z.rh])
        keep = iota((z.fj, z.rh), 0) // z.bs == iota((z.fj, z.rh), 1) % z.jl
        lt[jg] = jnp.where(keep, piece, 0.0).astype(BF)

    count(rg.at[pl.ds(0, z.n - z.mp)], rw_recv)
    right = None
    for dd in range(z.dp):
        part = dot_nn(rg[dd * z.mp:(dd + 1) * z.mp].reshape(z.mp * z.pad, z.orow), p1[dd])
        right = part if right is None else right + part
    right = right.astype(BF)
    for g in range(z.groups):
        for s in range(z.gs):
            shape = (z.ng, z.mp * z.pad)
            a, b = iota(shape, 0), iota(shape, 1)
            j = (a // z.nj) * z.jl + a % z.jl
            src = (a % z.nj) // (z.own * z.jl)
            pick = ones_where((src == s) & (b == (g * z.gs + s) * z.pad + j))
            piece = dot_nn(pick, right)
            shape = (z.ng, z.feat)
            keep = (iota(shape, 0) // z.jl) % z.own == iota(shape, 1) // z.bs
            wt[g, :, s * z.feat:(s + 1) * z.feat] = jnp.where(keep, piece, 0.0).astype(BF)

    @each_part
    def _(part):
        local_x(part).wait()
        local_c(part).wait()
        for s in range(1, chips):
            arrived(part, same_core(s))
            forward(part, chips + s, same_core(s)).start()
        arrived(part, partner)
        for s in range(1, chips):
            arrived(part, other_core(s))
        r = pl.ds(part[1], part[2])
        xs = [join([xfull[g * z.gs + s, r] for s in range(z.gs)]) for g in range(z.groups)]
        inner = [dot_nt(xs[g], wt[g]).astype(BF) for g in range(z.groups)]
        back = []
        for jg in range(z.jg):
            mixed = join([v[:, jg * z.nj:(jg + 1) * z.nj] for v in inner])
            pre = dot_nt(mixed, lt[jg])
            cdf = 0.5 * (1.0 + lax.erf(pre * 0.7071067811865476))
            slope = cdf + pre * (jnp.exp(-0.5 * pre * pre) * 0.3989422804014327)
            cols = pl.ds(jg * z.fj, z.fj)
            act[r, cols] = (pre * cdf).astype(BF)
            dpre = (cot[r, cols].astype(F32) * slope).astype(BF)
            glacc[jg] += dot_tn(dpre, mixed)
            back.append(dot_nn(dpre, lt[jg]).astype(BF))
        for g in range(z.groups):
            dinner = join([v[:, g * z.nj:(g + 1) * z.nj] for v in back])
            gracc[g] += dot_tn(dinner, xs[g])

    shape = (z.bs, z.fj)
    fold = ones_where(iota(shape, 1) % z.bs == iota(shape, 0))
    lefts = []
    for jg in range(z.jg):
        keep = iota((z.fj, z.rh), 0) // z.bs == iota((z.fj, z.rh), 1) % z.jl
        lefts.append(dot_nn(fold, jnp.where(keep, glacc[jg], 0.0).astype(BF)).astype(BF))
    left = join(lefts)
    for dd in range(z.dp):
        lsend[dd] = dot_nt(left, p2[dd]).astype(BF)

    @pl.loop(1, z.dp)
    def _(s):
        o = lax.rem(d + s, z.dp)
        pltpu.make_async_remote_copy(
            src_ref=lsend.at[o], dst_ref=lrecv.at[d], send_sem=gl_send, recv_sem=gl_recv,
            device_id=(o, p), device_id_type=MESH).start()

    pieces = []
    for g in range(z.groups):
        for s in range(z.gs):
            shape = (z.pad, z.ng)
            a, b = iota(shape, 0), iota(shape, 1)
            j = (b // z.nj) * z.jl + b % z.jl
            src = (b % z.nj) // (z.own * z.jl)
            pick = ones_where((src == s) & (a == j))
            shape = (z.ng, z.feat)
            keep = (iota(shape, 0) // z.jl) % z.own == iota(shape, 1) // z.bs
            piece = jnp.where(keep, gracc[g, :, s * z.feat:(s + 1) * z.feat], 0.0).astype(BF)
            pieces.append(dot_nn(pick, piece).astype(BF))
    pieces = join(pieces, axis=0)
    for dd in range(z.dp):
        owned = dot_nt(pieces, p1[dd]).astype(BF)
        rsend[dd * z.mp:(dd + 1) * z.mp] = owned.reshape(z.mp, z.pad, z.orow)

    @pl.loop(1, z.n)
    def _(s):
        o = lax.rem(me + s, z.n)
        pltpu.make_async_remote_copy(
            src_ref=rsend.at[o], dst_ref=rrecv.at[me], send_sem=gr_send, recv_sem=gr_recv,
            device_id=(o // z.mp, lax.rem(o, z.mp)), device_id_type=MESH).start()

    lrecv[d] = lsend[d]
    rrecv[me] = rsend[me]

    @each_part
    def _(part):
        for s in range(1, chips):
            send_own(part, s, same_core(s)).wait_send()
            forward(part, chips + s, same_core(s)).wait_send()
        send_own(part, 0, partner).wait_send()

    count(rg.at[pl.ds(0, z.mp - 1)], ra_send)
    count(rg.at[pl.ds(0, z.n - z.mp)], rw_send)
    count(lg.at[pl.ds(0, z.dp - 1)], lw_send)

    count(lrecv.at[pl.ds(0, z.dp - 1)], gl_recv)
    total = lrecv[0].astype(F32)
    for dd in range(1, z.dp):
        total = total + lrecv[dd].astype(F32)
    gl_ref[...] = total.T if z.direct else total
    count(rrecv.at[pl.ds(0, z.n - 1)], gr_recv)
    total = rrecv[0:z.mp].astype(F32)
    for dd in range(1, z.dp):
        total = total + rrecv[dd * z.mp:(dd + 1) * z.mp].astype(F32)
    gr_ref[...] = total.reshape(z.blocks, z.orow).T if z.direct else total
    count(lsend.at[pl.ds(0, z.dp - 1)], gl_send)
    count(rsend.at[pl.ds(0, z.n - 1)], gr_send)


def split_kernel(z, x_hbm, cot_hbm, rw_hbm, lw_hbm, act, gr_ref, gl_ref,
                 xfull, x2, cot, rw_v, lw_v, rwt, lwt, rg, rg2, lg, p1, p2, wt, wt2, lt, gracc, glacc,
                 isend, irecv, dsend, drecv, turn, esend, erecv, fsend, frecv, rsend, rrecv, final, lsend, lrecv,
                 x_recv, x_send, x_local, c_local, w_local, i_send, i_recv, d_send, d_recv,
                 e_send, e_recv, f_send, f_recv, gr_send, gr_recv,
                 rw_send, rw_recv, lw_send, lw_recv, gl_send, gl_recv, ra_send, ra_recv, rb_send, rb_recv, met):
    d, p = lax.axis_index("dp"), lax.axis_index("mp")
    me = d * z.mp + p
    core = lax.rem(p, 2)
    partner = p + 1 - 2 * core
    chip = p // 2
    chips = z.mp // 2
    n1, n2, tc = z.n1, z.n2, z.tc
    first = n1 * tc

    def same_core(s):
        return lax.rem(chip + s, chips) * 2 + core

    def other_core(s):
        return lax.rem(chip + s, chips) * 2 + 1 - core

    barrier = pltpu.get_barrier_semaphore()
    if z.cube:
        for s in range(1, z.mp):
            pl.semaphore_signal(barrier, inc=1, device_id=(d, lax.rem(p + s, z.mp)), device_id_type=MESH)
        for r in range(z.rounds):
            pl.semaphore_signal(barrier, inc=1, device_id=(across(d, r), p), device_id_type=MESH)
        near = z.mp - 1 + z.rounds
    else:
        @pl.loop(1, z.n)
        def _(s):
            o = lax.rem(me + s, z.n)
            pl.semaphore_signal(barrier, inc=1, device_id=(o // z.mp, lax.rem(o, z.mp)), device_id_type=MESH)
        near = z.n - 1

    def rows(c):
        return pl.ds(pl.multiple_of(c * tc, tc), tc)

    def later(c):
        return pl.ds(pl.multiple_of(first + c * tc, tc), tc)

    def local_x(c):
        return pltpu.make_async_copy(x_hbm.at[rows(c)], xfull.at[p, rows(c)], x_local.at[c])

    def local_x2(c):
        return pltpu.make_async_copy(x_hbm.at[later(c)], x2.at[rows(c)], x_local.at[n1 + c])

    def local_c(c):
        return pltpu.make_async_copy(cot_hbm.at[rows(c)], cot.at[rows(c)], c_local.at[c])

    def send_own(c, kind, target):
        return pltpu.make_async_remote_copy(
            src_ref=xfull.at[p, rows(c)], dst_ref=xfull.at[p, rows(c)],
            send_sem=x_send.at[kind, c], recv_sem=x_recv.at[p, c],
            device_id=(d, target), device_id_type=MESH)

    def forward(c, kind, source):
        return pltpu.make_async_remote_copy(
            src_ref=xfull.at[source, rows(c)], dst_ref=xfull.at[source, rows(c)],
            send_sem=x_send.at[kind, c], recv_sem=x_recv.at[source, c],
            device_id=(d, partner), device_id_type=MESH)

    def arrived(c, source):
        forward(c, 0, source).wait_recv()

    def each_mp(send):
        for s in range(1, chips):
            send(same_core(s))
            send(other_core(s))
        send(partner)

    def dinners(c, jg):
        for s in range(1, chips):
            send_dinner(c, jg, 1, same_core(s))
            send_dinner(c, jg, 1, other_core(s))
        send_dinner(c, jg, 0, partner)

    def send_inner(c, q):
        pltpu.make_async_remote_copy(
            src_ref=isend.at[q, rows(c)], dst_ref=irecv.at[p, rows(c)],
            send_sem=i_send.at[c], recv_sem=i_recv.at[c],
            device_id=(d, q), device_id_type=MESH).start()

    def send_dinner(c, jg, kind, q):
        pltpu.make_async_remote_copy(
            src_ref=dsend.at[jg, q, rows(c)], dst_ref=drecv.at[jg, p, rows(c)],
            send_sem=d_send.at[jg, c], recv_sem=d_recv.at[jg, kind, c],
            device_id=(d, q), device_id_type=MESH).start()

    def send_first(q):
        pltpu.make_async_remote_copy(
            src_ref=fsend.at[q], dst_ref=frecv.at[p], send_sem=f_send, recv_sem=f_recv,
            device_id=(d, q), device_id_type=MESH).start()

    def count(ref, sem):
        pltpu.make_async_copy(ref, ref, sem).wait()

    def others(ref):
        return ref.at[pl.ds(0, z.mp - 1)]

    @pl.loop(0, n1)
    def _(c):
        local_x(c).start()

    local_r = pltpu.make_async_copy(rw_hbm, rw_v, w_local.at[0])
    local_r.start()
    local_l = pltpu.make_async_copy(lw_hbm, lw_v, w_local.at[1])
    local_l.start()

    def send_x(c):
        local_x(c).wait()
        for s in range(1, chips):
            send_own(c, s, same_core(s)).start()
        send_own(c, 0, partner).start()

    pl.semaphore_wait(barrier, near)
    send_x(0)
    local_r.wait()
    local_l.wait()
    shape = (z.mp * z.pad, z.bs)
    a, b = iota(shape, 0), iota(shape, 1)
    wide = ones_where((a % z.pad < z.own) & (b == (a // z.pad) * z.own + a % z.pad))
    rwt[...] = dot_nt(wide, rw_v[...]).astype(BF).reshape(z.mp, z.pad, z.orow)
    shape = (z.bs, z.bs)
    lwt[...] = dot_nt(ones_where(iota(shape, 0) == iota(shape, 1)), lw_v[...]).astype(BF)
    rg[me] = rwt[p]
    rg2[d] = rwt[...]
    lg[d] = lwt[...]
    for s in range(1, z.mp):
        q = lax.rem(p + s, z.mp)
        pltpu.make_async_remote_copy(
            src_ref=rwt.at[q], dst_ref=rg.at[me], send_sem=ra_send, recv_sem=ra_recv,
            device_id=(d, q), device_id_type=MESH).start()

    @pl.loop(1, n1)
    def _(c):
        send_x(c)

    if z.cube:
        for r in range(z.rounds):
            pl.semaphore_signal(met.at[r], inc=1, device_id=(across(d, r), p), device_id_type=MESH)
            pl.semaphore_wait(met.at[r], 1)

    @pl.loop(0, n1)
    def _(c):
        local_c(c).start()

    @pl.loop(0, n2)
    def _(c):
        local_x2(c).start()
        local_c(n1 + c).start()

    @pl.loop(1, z.dp)
    def _(s):
        pltpu.make_async_remote_copy(
            src_ref=rwt, dst_ref=rg2.at[d], send_sem=rb_send, recv_sem=rb_recv,
            device_id=(lax.rem(d + s, z.dp), p), device_id_type=MESH).start()

    @pl.loop(1, z.dp)
    def _(s):
        pltpu.make_async_remote_copy(
            src_ref=lwt, dst_ref=lg.at[d], send_sem=lw_send, recv_sem=lw_recv,
            device_id=(lax.rem(d + s, z.dp), p), device_id_type=MESH).start()

    count(others(rg), ra_recv)
    mine = rg.at[pl.ds(d * z.mp, z.mp)]

    @pl.loop(1, z.dp)
    def _(s):
        pltpu.make_async_remote_copy(
            src_ref=mine, dst_ref=mine, send_sem=rw_send, recv_sem=rw_recv,
            device_id=(lax.rem(d + s, z.dp), p), device_id_type=MESH).start()

    for dd in range(z.dp):
        shape = (z.orow, z.feat)
        a, b = iota(shape, 0), iota(shape, 1)
        source = (b // z.bs) * z.rows + (b % z.bs) - dd * z.rows
        inside = (b % z.bs) // z.rows == dd
        p1[dd] = ones_where(inside & (a == source))
        shape = (z.orow, z.blocks * z.own)
        a, b = iota(shape, 0), iota(shape, 1)
        jg = b // z.rh
        i_all = (b % z.rh) // z.jl
        j = jg * z.jl + b % z.jl
        inside = i_all // z.rows == dd
        p2[dd] = ones_where(inside & (a == j * z.rows + i_all % z.rows))
    for a in range(z.quads):
        shape = (256, 256)
        u, v = iota(shape, 0), iota(shape, 1)
        owner = (u % z.bs) // z.rows
        slot = (v % 128) // z.unit
        same = (u // z.bs == (v % z.unit) // z.rows) & (u % z.rows == v % z.rows)
        turn[a] = ones_where(same & (owner // z.slots == v // 128) & ((owner + a) % z.slots == slot))
    gracc[...] = jnp.zeros_like(gracc)
    glacc[...] = jnp.zeros_like(glacc)

    def expand(blocks, target):
        right = None
        for dd in range(z.dp):
            part = dot_nn(blocks(dd).reshape(z.mp * z.pad, z.orow), p1[dd])
            right = part if right is None else right + part
        right = right.astype(BF)
        for g in range(z.mp):
            shape = (z.ng, z.mp * z.pad)
            a, b = iota(shape, 0), iota(shape, 1)
            pick = ones_where(b == g * z.pad + (a // z.nj) * z.jl + a % z.jl)
            piece = dot_nn(pick, right)
            shape = (z.ng, z.feat)
            keep = (iota(shape, 0) // z.jl) % z.own == iota(shape, 1) // z.bs
            target[g] = jnp.where(keep, piece, 0.0).astype(BF)

    count(rg2.at[pl.ds(0, z.dp - 1)], rb_recv)
    expand(lambda dd: rg2[dd], wt2)

    @pl.loop(0, n2)
    def _(c):
        local_x2(c).wait()
        own = x2[rows(c)]
        for q in range(z.mp):
            isend[q, rows(c)] = dot_nt(own, wt2[q]).astype(BF)
        each_mp(functools.partial(send_inner, c))
        irecv[p, rows(c)] = isend[p, rows(c)]
        for a in range(z.quads):
            cols = slice(a * 256, (a + 1) * 256)
            x2[rows(c), cols] = dot_nn(own[:, cols], turn[a]).astype(BF)

    def pass_on(c):
        for s in range(1, chips):
            arrived(c, same_core(s))
            forward(c, chips + s, same_core(s)).start()

    for c in range(z.early):
        pass_on(c)

    count(lg.at[pl.ds(0, z.dp - 1)], lw_recv)
    left = None
    for dd in range(z.dp):
        part = dot_nn(lg[dd], p2[dd])
        left = part if left is None else left + part
    left = left.astype(BF)
    shape = (z.fj, z.bs)
    spread = ones_where(iota(shape, 0) % z.bs == iota(shape, 1))
    for jg in range(z.jg):
        piece = dot_nn(spread, left[:, jg * z.rh:(jg + 1) * z.rh])
        keep = iota((z.fj, z.rh), 0) // z.bs == iota((z.fj, z.rh), 1) % z.jl
        lt[jg] = jnp.where(keep, piece, 0.0).astype(BF)

    count(rg.at[pl.ds(0, z.n - z.mp)], rw_recv)
    expand(lambda dd: rg[dd * z.mp:(dd + 1) * z.mp], wt)

    def layer(inner, r):
        back = []
        for jg in range(z.jg):
            mixed = join([v[:, jg * z.nj:(jg + 1) * z.nj] for v in inner])
            pre = dot_nt(mixed, lt[jg])
            cdf = 0.5 * (1.0 + lax.erf(pre * 0.7071067811865476))
            slope = cdf + pre * (jnp.exp(-0.5 * pre * pre) * 0.3989422804014327)
            cols = pl.ds(jg * z.fj, z.fj)
            act[r, cols] = (pre * cdf).astype(BF)
            dpre = (cot[r, cols].astype(F32) * slope).astype(BF)
            glacc[jg] += dot_tn(dpre, mixed)
            back.append(dot_nn(dpre, lt[jg]).astype(BF))
        return back

    @pl.loop(0, n1)
    def _(c):
        local_c(c).wait()
        @pl.when(c >= z.early)
        def _():
            pass_on(c)

        arrived(c, partner)
        for s in range(1, chips):
            arrived(c, other_core(s))
        r = rows(c)
        xs = [xfull[g, r] for g in range(z.mp)]
        back = layer([dot_nt(xs[g], wt[g]).astype(BF) for g in range(z.mp)], r)
        for g in range(z.mp):
            dinner = join([v[:, g * z.nj:(g + 1) * z.nj] for v in back])
            gracc[g] += dot_tn(dinner, xs[g])

    per = 128 // z.bs
    lane = iota((z.jl, 128), 1) // z.bs

    def diagonal(tile):
        parts = []
        for v in range(z.own // per):
            piece = tile(v * per, v)
            for w in range(1, per):
                piece = jnp.where(lane == w, tile(v * per + w, v), piece)
            parts.append(piece)
        return join(parts)

    pieces = []
    for g in range(z.mp):
        for jg in range(z.jg):
            pieces.append(diagonal(lambda i, v: gracc[
                g, jg * z.nj + i * z.jl:jg * z.nj + (i + 1) * z.jl, v * 128:(v + 1) * 128]))
    pieces = join(pieces, axis=0).astype(BF)
    for dd in range(z.dp):
        esend[dd] = dot_nt(pieces, p1[dd]).astype(BF)

    @pl.loop(1, z.dp)
    def _(s):
        o = lax.rem(d + s, z.dp)
        pltpu.make_async_remote_copy(
            src_ref=esend.at[o], dst_ref=erecv.at[d], send_sem=e_send, recv_sem=e_recv,
            device_id=(o, p), device_id_type=MESH).start()
    erecv[d] = esend[d]

    @pl.loop(0, n2)
    def _(c):
        local_c(n1 + c).wait()
        r = rows(c)
        count(irecv.at[pl.ds(0, z.mp - 1), r], i_recv.at[c])
        back = layer([irecv[g, r] for g in range(z.mp)], later(c))
        for jg in range(z.jg):
            for g in range(z.mp):
                dsend[jg, g, r] = back[jg][:, g * z.nj:(g + 1) * z.nj]
            drecv[jg, p, r] = dsend[jg, p, r]
        dinners(c, 0)

    for jg in range(1, z.jg):
        @pl.loop(0, n2)
        def _(c):
            dinners(c, jg)

    shape = (z.bs, z.fj)
    fold = ones_where(iota(shape, 1) % z.bs == iota(shape, 0))
    lefts = []
    for jg in range(z.jg):
        keep = iota((z.fj, z.rh), 0) // z.bs == iota((z.fj, z.rh), 1) % z.jl
        lefts.append(dot_nn(fold, jnp.where(keep, glacc[jg], 0.0).astype(BF)).astype(BF))
    left = join(lefts)
    for dd in range(z.dp):
        lsend[dd] = dot_nt(left, p2[dd]).astype(BF)

    @pl.loop(1, z.dp)
    def _(s):
        o = lax.rem(d + s, z.dp)
        pltpu.make_async_remote_copy(
            src_ref=lsend.at[o], dst_ref=lrecv.at[d], send_sem=gl_send, recv_sem=gl_recv,
            device_id=(o, p), device_id_type=MESH).start()
    lrecv[d] = lsend[d]

    count(erecv.at[pl.ds(0, z.dp - 1)], e_recv)
    total = erecv[0].astype(F32)
    for dd in range(1, z.dp):
        total = total + erecv[dd].astype(F32)
    fsend[...] = total.astype(BF).reshape(z.mp, z.own, z.orow)
    each_mp(send_first)
    frecv[p] = fsend[p]

    shape = (z.jl, 128)
    block_of = (iota(shape, 1) % z.unit) // z.rows
    slot_of = iota(shape, 1) // z.unit

    def pick(options, which):
        out = options[0]
        for w in range(1, len(options)):
            out = jnp.where(which == w, options[w], out)
        return out

    def owned(jg, s, lo, hi):
        base = lax.rem(chip + s, chips) * 2
        turned = [drecv[jg, base + k, lo * tc:hi * tc].T for k in range(2)]
        m = z.quad * z.jl
        tiles = []
        for a in range(z.quads):
            lhs = join([t[a * m:(a + 1) * m] for t in turned], axis=0)
            full = dot_nn(lhs, x2[lo * tc:hi * tc, a * 256:(a + 1) * 256])
            tiles.append([[pick([full[k * m + w * z.jl:k * m + (w + 1) * z.jl, h * 128:(h + 1) * 128]
                                 for w in range(z.quad)], block_of) for k in range(2)] for h in range(256 // 128)])
        out = []
        for dd in range(z.dp):
            h, t = dd // z.slots, dd % z.slots
            out.append(join([pick([tiles[(w - t) % z.slots][h][k] for w in range(z.slots)], slot_of)
                             for k in range(2)], axis=0))
        return out

    def exchange(unit, blocks):
        for dd in range(z.dp):
            rsend[unit, dd] = blocks[dd].astype(BF)

        @pl.loop(1, z.dp)
        def _(s):
            o = lax.rem(d + s, z.dp)
            pltpu.make_async_remote_copy(
                src_ref=rsend.at[unit, o], dst_ref=rrecv.at[unit, d],
                send_sem=gr_send.at[unit], recv_sem=gr_recv.at[unit],
                device_id=(o, p), device_id_type=MESH).start()
        rrecv[unit, d] = rsend[unit, d]

    def landed(jg, kind, lo, hi):
        for c in range(lo, hi):
            amount = z.mp - 2 if kind else 1
            count(drecv.at[jg, pl.ds(0, amount), pl.ds(c * tc, tc)], d_recv.at[jg, kind, c])

    units = [(jg, s) for s in range(chips) for jg in range(z.jg)]
    for s in range(chips):
        for jg in range(z.jg):
            unit = units.index((jg, s))
            if s == 1 and jg == z.jg - 1 and n2 > 1:
                landed(jg, 1, 0, n2 - 1)
                early = owned(jg, s, 0, n2 - 1)
                landed(jg, 1, n2 - 1, n2)
                late = owned(jg, s, n2 - 1, n2)
                exchange(unit, [u + v for u, v in zip(early, late)])
            else:
                if s < 2:
                    landed(jg, s, 0, n2)
                exchange(unit, owned(jg, s, 0, n2))

    @pl.loop(0, n1)
    def _(c):
        for s in range(1, chips):
            send_own(c, s, same_core(s)).wait_send()
            forward(c, chips + s, same_core(s)).wait_send()
        send_own(c, 0, partner).wait_send()

    @pl.loop(0, n2)
    def _(c):
        count(isend.at[pl.ds(0, z.mp - 1), rows(c)], i_send.at[c])
        for jg in range(z.jg):
            count(dsend.at[jg, pl.ds(0, z.mp - 1), rows(c)], d_send.at[jg, c])

    count(others(rg), ra_send)
    count(esend.at[pl.ds(0, z.dp - 1)], e_send)
    count(others(fsend), f_send)
    count(rg.at[pl.ds(0, z.n - z.mp)], rw_send)
    count(rg2.at[pl.ds(0, z.dp - 1)], rb_send)
    count(lg.at[pl.ds(0, z.dp - 1)], lw_send)

    count(lrecv.at[pl.ds(0, z.dp - 1)], gl_recv)
    total = lrecv[0].astype(F32)
    for dd in range(1, z.dp):
        total = total + lrecv[dd].astype(F32)
    gl_ref[...] = total.T
    count(others(frecv), f_recv)
    spin = lax.rem(128 - lax.rem(d, z.slots) * z.unit, 128)
    for unit, (jg, s) in enumerate(units):
        count(rrecv.at[unit, pl.ds(0, z.dp - 1)], gr_recv.at[unit])
        total = rrecv[unit, 0].astype(F32)
        for dd in range(1, z.dp):
            total = total + rrecv[unit, dd].astype(F32)
        total = pltpu.roll(total, spin, 1)
        for k in range(2):
            final[lax.rem(chip + s, chips) * 2 + k, jg] = total[k * z.jl:(k + 1) * z.jl]
    total = final[...].reshape(z.blocks, z.orow) + frecv[...].astype(F32).reshape(z.blocks, z.orow)
    gr_ref[...] = total.T
    count(lsend.at[pl.ds(0, z.dp - 1)], gl_send)
    for unit in range(len(units)):
        count(rsend.at[unit, pl.ds(0, z.dp - 1)], gr_send.at[unit])


def split_scratch(z):
    dma = pltpu.SemaphoreType.DMA
    return [
        pltpu.VMEM((z.mp, z.n1 * z.tc, z.feat), BF),
        pltpu.VMEM((z.n2 * z.tc, z.feat), BF),
        pltpu.VMEM((z.tok, z.feat), BF),
        pltpu.VMEM((z.orow, z.bs), BF),
        pltpu.VMEM((z.orow, z.bs), BF),
        pltpu.VMEM((z.mp, z.pad, z.orow), BF),
        pltpu.VMEM((z.bs, z.orow), BF),
        pltpu.VMEM((z.n, z.pad, z.orow), BF),
        pltpu.VMEM((z.dp, z.mp, z.pad, z.orow), BF),
        pltpu.VMEM((z.dp, z.bs, z.orow), BF),
        pltpu.VMEM((z.dp, z.orow, z.feat), BF),
        pltpu.VMEM((z.dp, z.orow, z.blocks * z.own), BF),
        pltpu.VMEM((z.mp, z.ng, z.feat), BF),
        pltpu.VMEM((z.mp, z.ng, z.feat), BF),
        pltpu.VMEM((z.jg, z.fj, z.rh), BF),
        pltpu.VMEM((z.mp, z.ng, z.feat), F32),
        pltpu.VMEM((z.jg, z.fj, z.rh), F32),
        pltpu.VMEM((z.mp, z.n2 * z.tc, z.ng), BF),
        pltpu.VMEM((z.mp, z.n2 * z.tc, z.ng), BF),
        pltpu.VMEM((z.jg, z.mp, z.n2 * z.tc, z.nj), BF),
        pltpu.VMEM((z.jg, z.mp, z.n2 * z.tc, z.nj), BF),
        pltpu.VMEM((z.quads, 256, 256), BF),
        pltpu.VMEM((z.dp, z.blocks, z.orow), BF),
        pltpu.VMEM((z.dp, z.blocks, z.orow), BF),
        pltpu.VMEM((z.mp, z.own, z.orow), BF),
        pltpu.VMEM((z.mp, z.own, z.orow), BF),
        pltpu.VMEM((z.units, z.dp, 2 * z.jl, z.orow), BF),
        pltpu.VMEM((z.units, z.dp, 2 * z.jl, z.orow), BF),
        pltpu.VMEM((z.mp, z.jg, z.jl, z.orow), F32),
        pltpu.VMEM((z.dp, z.bs, z.orow), BF),
        pltpu.VMEM((z.dp, z.bs, z.orow), BF),
        dma((z.mp, z.n1)),
        dma((z.mp, z.n1)),
        dma((CHUNKS,)),
        dma((CHUNKS,)),
        dma((2,)),
        dma((z.n2,)),
        dma((z.n2,)),
        dma((z.jg, z.n2)),
        dma((z.jg, 2, z.n2)),
        dma, dma, dma, dma,
        dma((z.units,)),
        dma((z.units,)),
        dma, dma, dma, dma, dma, dma, dma, dma, dma, dma,
        pltpu.SemaphoreType.REGULAR((max(1, z.rounds),)),
    ]


def store(act, gr, gl, act_out, gr_out, gl_out, sems):
    size = act.shape[0] // CHUNKS
    copies = [pltpu.make_async_copy(gr, gr_out, sems.at[0]), pltpu.make_async_copy(gl, gl_out, sems.at[1])]
    for c in range(CHUNKS):
        r = pl.ds(c * size, size)
        copies.append(pltpu.make_async_copy(act.at[r], act_out.at[r], sems.at[2 + c]))
    for copy in copies:
        copy.start()
    for copy in copies:
        copy.wait()


def shards(z, tokens, right_weight, left_weight, cotangent):
    rw = right_weight.reshape(z.orow, z.bs)
    lw = left_weight.reshape(z.orow, z.bs)
    hbm = pl.BlockSpec(memory_space=pltpu.HBM)
    vmem = pl.BlockSpec(memory_space=pltpu.VMEM)
    dma = pltpu.SemaphoreType.DMA
    act, gr, gl = pl.pallas_call(
        functools.partial(split_kernel if z.split else kernel, z),
        out_shape=(
            pltpu.VMEM((z.tok, z.feat), BF),
            pltpu.VMEM((z.orow, z.bs) if z.direct else (z.mp, z.pad, z.orow), F32),
            pltpu.VMEM((z.orow, z.bs) if z.direct else (z.bs, z.orow), F32),
        ),
        in_specs=[hbm] * 4,
        out_specs=(vmem, vmem, vmem),
        scratch_shapes=split_scratch(z) if z.split else [
            pltpu.VMEM((z.mp, z.tok, z.feat), BF),
            pltpu.VMEM((z.tok, z.feat), BF),
            pltpu.VMEM((z.orow, z.bs), BF),
            pltpu.VMEM((z.orow, z.bs), BF),
            pltpu.VMEM((z.mp, z.pad, z.orow), BF),
            pltpu.VMEM((z.bs, z.orow), BF),
            pltpu.VMEM((z.n, z.pad, z.orow), BF),
            pltpu.VMEM((z.dp, z.bs, z.orow), BF),
            pltpu.VMEM((z.dp, z.orow, z.feat), BF),
            pltpu.VMEM((z.dp, z.orow, z.blocks * z.own), BF),
            pltpu.VMEM((z.groups, z.ng, z.kg), BF),
            pltpu.VMEM((z.jg, z.fj, z.rh), BF),
            pltpu.VMEM((z.groups, z.ng, z.kg), F32),
            pltpu.VMEM((z.jg, z.fj, z.rh), F32),
            pltpu.VMEM((z.n, z.pad, z.orow), BF),
            pltpu.VMEM((z.n, z.pad, z.orow), BF),
            pltpu.VMEM((z.dp, z.bs, z.orow), BF),
            pltpu.VMEM((z.dp, z.bs, z.orow), BF),
            dma((z.mp, z.parts)),
            dma((z.mp, z.parts)),
            dma((z.parts,)),
            dma((z.parts,)),
            dma((2,)),
            dma, dma, dma, dma, dma, dma, dma, dma, dma, dma,
            pltpu.SemaphoreType.REGULAR((max(1, z.rounds),)),
        ],
        compiler_params=pltpu.CompilerParams(
            collective_id=0, has_side_effects=True, vmem_limit_bytes=61 * 1024 * 1024),
    )(tokens, cotangent, rw, lw)
    act, gr, gl = pl.pallas_call(
        store,
        out_shape=[jax.ShapeDtypeStruct(v.shape, v.dtype) for v in (act, gr, gl)],
        in_specs=[vmem] * 3,
        out_specs=[hbm] * 3,
        scratch_shapes=[dma((2 + CHUNKS,))],
        compiler_params=pltpu.CompilerParams(vmem_limit_bytes=1024 * 1024),
    )(act, gr, gl)
    if z.direct:
        return act, gr.reshape(z.own, z.rows, z.bs), gl.reshape(z.own, z.rows, z.bs)
    gr = gr[:, :z.own].reshape(z.mp * z.own, z.own, z.rows).transpose(1, 2, 0)
    gl = gl.reshape(z.bs, z.own, z.rows).transpose(1, 2, 0)
    return act, gr, gl


def solution(mesh):
    n_dp, n_mp = mesh.shape["dp"], mesh.shape["mp"]

    def step(tokens, right_weight, left_weight, cotangent):
        z = Sizes(n_dp, n_mp, tokens.shape[0] // n_dp, tokens.shape[1] // n_mp, right_weight.shape[1])
        return jax.shard_map(
            functools.partial(shards, z),
            mesh=mesh,
            in_specs=(P("dp", "mp"), P("mp", "dp", None), P("mp", "dp", None), P("dp", "mp")),
            out_specs=(P("dp", "mp"), P("mp", "dp", None), P("mp", "dp", None)),
            check_vma=False,
        )(tokens, right_weight, left_weight, cotangent)

    return step
```

```python
import functools

import jax
import jax.numpy as jnp
from jax import lax
from jax.experimental import pallas as pl
from jax.experimental.pallas import tpu as pltpu
from jax.sharding import PartitionSpec as P

MESH = pl.DeviceIdType.MESH
BF = jnp.bfloat16
F32 = jnp.float32
CHUNKS = 8
TAIL = (1,)


def iota(shape, dim):
    line = tuple(n if axis == dim else 1 for axis, n in enumerate(shape))
    return lax.broadcasted_iota(jnp.int32, line, dim)


def ones_where(cond):
    return jnp.where(cond, 1.0, 0.0).astype(BF)


def dot_nn(a, b):
    return lax.dot_general(a, b, (((1,), (0,)), ((), ())), preferred_element_type=F32)


def dot_nt(a, b):
    return lax.dot_general(a, b, (((1,), (1,)), ((), ())), preferred_element_type=F32)


def dot_tn(a, b):
    return lax.dot_general(a, b, (((0,), (0,)), ((), ())), preferred_element_type=F32)


def join(parts, axis=1):
    return parts[0] if len(parts) == 1 else jnp.concatenate(parts, axis=axis)


def across(index, r):
    bit = 1 << r
    return index + bit - 2 * bit * lax.rem(index // bit, 2)


class Sizes:
    def __init__(self, n_dp, n_mp, tok_rows, features, width):
        self.dp, self.mp = n_dp, n_mp
        self.tok, self.feat, self.bs = tok_rows, features, width
        self.own = features // width
        self.blocks = self.own * n_mp
        self.rows = width // n_dp
        self.orow = self.own * self.rows
        self.pad = max(self.own, 16)
        self.gs = max(1, 128 // (self.own * self.own))
        self.groups = n_mp // self.gs
        self.ng = self.gs * self.own * self.own
        self.kg = self.gs * features
        self.jg = self.ng // 128
        self.jl = self.own // self.jg
        self.nj = self.ng // self.jg
        self.rh = self.groups * self.nj
        self.fj = self.jl * width
        self.n = n_dp * n_mp
        self.direct = self.pad == self.own and self.orow % 128 == 0
        self.tc = tok_rows // CHUNKS
        self.main = CHUNKS - 1
        self.tail = []
        start = self.main * self.tc
        for part in TAIL:
            self.tail.append((self.main + len(self.tail), start, self.tc // part))
            start += self.tc // part
        self.parts = self.main + len(self.tail)
        self.n1 = CHUNKS // 2
        self.n2 = CHUNKS - self.n1
        self.early = min(2, self.n1)
        self.quad = 256 // width
        self.quads = self.own // max(1, self.quad)
        self.unit = self.quad * self.rows
        self.slots = 128 // self.unit
        self.split = self.gs == 1 and self.jl == 8 and self.rows == 8 and self.orow == 128 and width == 64 and n_mp == 4 and self.jg == 2
        self.rounds = n_dp.bit_length() - 1
        self.cube = n_dp == 1 << self.rounds


def kernel(z, x_hbm, cot_hbm, rw_hbm, lw_hbm, act, gr_ref, gl_ref,
           xfull, cot, rw_v, lw_v, rwt, lwt, rg, lg, p1, p2, wt, lt, gracc, glacc,
           rsend, rrecv, lsend, lrecv,
           x_recv, x_send, x_local, c_local, w_local,
           rw_send, rw_recv, lw_send, lw_recv, gr_send, gr_recv, gl_send, gl_recv, ra_send, ra_recv, met):
    d, p = lax.axis_index("dp"), lax.axis_index("mp")
    me = d * z.mp + p
    core = lax.rem(p, 2)
    partner = p + 1 - 2 * core
    chip = p // 2
    chips = z.mp // 2

    def same_core(s):
        return lax.rem(chip + s, chips) * 2 + core

    def other_core(s):
        return lax.rem(chip + s, chips) * 2 + 1 - core

    barrier = pltpu.get_barrier_semaphore()
    if z.cube:
        for s in range(1, z.mp):
            pl.semaphore_signal(barrier, inc=1, device_id=(d, lax.rem(p + s, z.mp)), device_id_type=MESH)
        for r in range(z.rounds):
            pl.semaphore_signal(barrier, inc=1, device_id=(across(d, r), p), device_id_type=MESH)
        near = z.mp - 1 + z.rounds
    else:
        @pl.loop(1, z.n)
        def _(s):
            o = lax.rem(me + s, z.n)
            pl.semaphore_signal(barrier, inc=1, device_id=(o // z.mp, lax.rem(o, z.mp)), device_id_type=MESH)
        near = z.n - 1

    def full(c):
        return c, pl.multiple_of(c * z.tc, z.tc), z.tc

    def local_x(part):
        c, start, size = part
        return pltpu.make_async_copy(x_hbm.at[pl.ds(start, size)], xfull.at[p, pl.ds(start, size)], x_local.at[c])

    def local_c(part):
        c, start, size = part
        return pltpu.make_async_copy(cot_hbm.at[pl.ds(start, size)], cot.at[pl.ds(start, size)], c_local.at[c])

    def send_own(part, kind, target):
        c, start, size = part
        return pltpu.make_async_remote_copy(
            src_ref=x_hbm.at[pl.ds(start, size)], dst_ref=xfull.at[p, pl.ds(start, size)],
            send_sem=x_send.at[kind, c], recv_sem=x_recv.at[p, c],
            device_id=(d, target), device_id_type=MESH)

    def forward(part, kind, source):
        c, start, size = part
        return pltpu.make_async_remote_copy(
            src_ref=xfull.at[source, pl.ds(start, size)], dst_ref=xfull.at[source, pl.ds(start, size)],
            send_sem=x_send.at[kind, c], recv_sem=x_recv.at[source, c],
            device_id=(d, partner), device_id_type=MESH)

    def arrived(part, source):
        c, start, size = part
        pltpu.make_async_remote_copy(
            src_ref=xfull.at[source, pl.ds(start, size)], dst_ref=xfull.at[source, pl.ds(start, size)],
            send_sem=x_send.at[0, c], recv_sem=x_recv.at[source, c],
            device_id=(d, partner), device_id_type=MESH).wait_recv()

    def each_part(step, first=0):
        @pl.loop(first, z.main)
        def _(c):
            step(full(c))
        for part in z.tail:
            step(part)

    local_r = pltpu.make_async_copy(rw_hbm, rw_v, w_local.at[0])
    local_r.start()
    local_l = pltpu.make_async_copy(lw_hbm, lw_v, w_local.at[1])
    local_l.start()

    local_r.wait()
    local_l.wait()
    shape = (z.mp * z.pad, z.bs)
    a, b = iota(shape, 0), iota(shape, 1)
    wide = ones_where((a % z.pad < z.own) & (b == (a // z.pad) * z.own + a % z.pad))
    rwt[...] = dot_nt(wide, rw_v[...]).astype(BF).reshape(z.mp, z.pad, z.orow)
    shape = (z.bs, z.bs)
    lwt[...] = dot_nt(ones_where(iota(shape, 0) == iota(shape, 1)), lw_v[...]).astype(BF)
    rg[me] = rwt[p]
    lg[d] = lwt[...]

    pl.semaphore_wait(barrier, near)

    def send_x(part):
        for s in range(1, chips):
            send_own(part, s, same_core(s)).start()
        send_own(part, 0, partner).start()

    for s in range(1, z.mp):
        q = lax.rem(p + s, z.mp)
        pltpu.make_async_remote_copy(
            src_ref=rwt.at[q], dst_ref=rg.at[me], send_sem=ra_send, recv_sem=ra_recv,
            device_id=(d, q), device_id_type=MESH).start()

    each_part(send_x)

    if z.cube:
        for r in range(z.rounds):
            pl.semaphore_signal(met.at[r], inc=1, device_id=(across(d, r), p), device_id_type=MESH)
            pl.semaphore_wait(met.at[r], 1)

    @each_part
    def _(part):
        local_x(part).start()
        local_c(part).start()

    def count(ref, sem):
        pltpu.make_async_copy(ref, ref, sem).wait()

    @pl.loop(1, z.dp)
    def _(s):
        pltpu.make_async_remote_copy(
            src_ref=lwt, dst_ref=lg.at[d], send_sem=lw_send, recv_sem=lw_recv,
            device_id=(lax.rem(d + s, z.dp), p), device_id_type=MESH).start()

    count(rg.at[pl.ds(0, z.mp - 1)], ra_recv)
    mine = rg.at[pl.ds(d * z.mp, z.mp)]

    @pl.loop(1, z.dp)
    def _(s):
        pltpu.make_async_remote_copy(
            src_ref=mine, dst_ref=mine, send_sem=rw_send, recv_sem=rw_recv,
            device_id=(lax.rem(d + s, z.dp), p), device_id_type=MESH).start()

    for dd in range(z.dp):
        shape = (z.orow, z.feat)
        a, b = iota(shape, 0), iota(shape, 1)
        source = (b // z.bs) * z.rows + (b % z.bs) - dd * z.rows
        inside = (b % z.bs) // z.rows == dd
        p1[dd] = ones_where(inside & (a == source))
        shape = (z.orow, z.blocks * z.own)
        a, b = iota(shape, 0), iota(shape, 1)
        jg = b // z.rh
        i_all = (b % z.rh) // z.jl
        j = jg * z.jl + b % z.jl
        inside = i_all // z.rows == dd
        p2[dd] = ones_where(inside & (a == j * z.rows + i_all % z.rows))
    gracc[...] = jnp.zeros_like(gracc)
    glacc[...] = jnp.zeros_like(glacc)

    count(lg.at[pl.ds(0, z.dp - 1)], lw_recv)
    left = None
    for dd in range(z.dp):
        part = dot_nn(lg[dd], p2[dd])
        left = part if left is None else left + part
    left = left.astype(BF)
    shape = (z.fj, z.bs)
    spread = ones_where(iota(shape, 0) % z.bs == iota(shape, 1))
    for jg in range(z.jg):
        piece = dot_nn(spread, left[:, jg * z.rh:(jg + 1) * z.rh])
        keep = iota((z.fj, z.rh), 0) // z.bs == iota((z.fj, z.rh), 1) % z.jl
        lt[jg] = jnp.where(keep, piece, 0.0).astype(BF)

    count(rg.at[pl.ds(0, z.n - z.mp)], rw_recv)
    right = None
    for dd in range(z.dp):
        part = dot_nn(rg[dd * z.mp:(dd + 1) * z.mp].reshape(z.mp * z.pad, z.orow), p1[dd])
        right = part if right is None else right + part
    right = right.astype(BF)
    for g in range(z.groups):
        for s in range(z.gs):
            shape = (z.ng, z.mp * z.pad)
            a, b = iota(shape, 0), iota(shape, 1)
            j = (a // z.nj) * z.jl + a % z.jl
            src = (a % z.nj) // (z.own * z.jl)
            pick = ones_where((src == s) & (b == (g * z.gs + s) * z.pad + j))
            piece = dot_nn(pick, right)
            shape = (z.ng, z.feat)
            keep = (iota(shape, 0) // z.jl) % z.own == iota(shape, 1) // z.bs
            wt[g, :, s * z.feat:(s + 1) * z.feat] = jnp.where(keep, piece, 0.0).astype(BF)

    @each_part
    def _(part):
        local_x(part).wait()
        local_c(part).wait()
        for s in range(1, chips):
            arrived(part, same_core(s))
            forward(part, chips + s, same_core(s)).start()
        arrived(part, partner)
        for s in range(1, chips):
            arrived(part, other_core(s))
        r = pl.ds(part[1], part[2])
        xs = [join([xfull[g * z.gs + s, r] for s in range(z.gs)]) for g in range(z.groups)]
        inner = [dot_nt(xs[g], wt[g]).astype(BF) for g in range(z.groups)]
        back = []
        for jg in range(z.jg):
            mixed = join([v[:, jg * z.nj:(jg + 1) * z.nj] for v in inner])
            pre = dot_nt(mixed, lt[jg])
            cdf = 0.5 * (1.0 + lax.erf(pre * 0.7071067811865476))
            slope = cdf + pre * (jnp.exp(-0.5 * pre * pre) * 0.3989422804014327)
            cols = pl.ds(jg * z.fj, z.fj)
            act[r, cols] = (pre * cdf).astype(BF)
            dpre = (cot[r, cols].astype(F32) * slope).astype(BF)
            glacc[jg] += dot_tn(dpre, mixed)
            back.append(dot_nn(dpre, lt[jg]).astype(BF))
        for g in range(z.groups):
            dinner = join([v[:, g * z.nj:(g + 1) * z.nj] for v in back])
            gracc[g] += dot_tn(dinner, xs[g])

    shape = (z.bs, z.fj)
    fold = ones_where(iota(shape, 1) % z.bs == iota(shape, 0))
    lefts = []
    for jg in range(z.jg):
        keep = iota((z.fj, z.rh), 0) // z.bs == iota((z.fj, z.rh), 1) % z.jl
        lefts.append(dot_nn(fold, jnp.where(keep, glacc[jg], 0.0).astype(BF)).astype(BF))
    left = join(lefts)
    for dd in range(z.dp):
        lsend[dd] = dot_nt(left, p2[dd]).astype(BF)

    @pl.loop(1, z.dp)
    def _(s):
        o = lax.rem(d + s, z.dp)
        pltpu.make_async_remote_copy(
            src_ref=lsend.at[o], dst_ref=lrecv.at[d], send_sem=gl_send, recv_sem=gl_recv,
            device_id=(o, p), device_id_type=MESH).start()

    pieces = []
    for g in range(z.groups):
        for s in range(z.gs):
            shape = (z.pad, z.ng)
            a, b = iota(shape, 0), iota(shape, 1)
            j = (b // z.nj) * z.jl + b % z.jl
            src = (b % z.nj) // (z.own * z.jl)
            pick = ones_where((src == s) & (a == j))
            shape = (z.ng, z.feat)
            keep = (iota(shape, 0) // z.jl) % z.own == iota(shape, 1) // z.bs
            piece = jnp.where(keep, gracc[g, :, s * z.feat:(s + 1) * z.feat], 0.0).astype(BF)
            pieces.append(dot_nn(pick, piece).astype(BF))
    pieces = join(pieces, axis=0)
    for dd in range(z.dp):
        owned = dot_nt(pieces, p1[dd]).astype(BF)
        rsend[dd * z.mp:(dd + 1) * z.mp] = owned.reshape(z.mp, z.pad, z.orow)

    @pl.loop(1, z.n)
    def _(s):
        o = lax.rem(me + s, z.n)
        pltpu.make_async_remote_copy(
            src_ref=rsend.at[o], dst_ref=rrecv.at[me], send_sem=gr_send, recv_sem=gr_recv,
            device_id=(o // z.mp, lax.rem(o, z.mp)), device_id_type=MESH).start()

    lrecv[d] = lsend[d]
    rrecv[me] = rsend[me]

    @each_part
    def _(part):
        for s in range(1, chips):
            send_own(part, s, same_core(s)).wait_send()
            forward(part, chips + s, same_core(s)).wait_send()
        send_own(part, 0, partner).wait_send()

    count(rg.at[pl.ds(0, z.mp - 1)], ra_send)
    count(rg.at[pl.ds(0, z.n - z.mp)], rw_send)
    count(lg.at[pl.ds(0, z.dp - 1)], lw_send)

    count(lrecv.at[pl.ds(0, z.dp - 1)], gl_recv)
    total = lrecv[0].astype(F32)
    for dd in range(1, z.dp):
        total = total + lrecv[dd].astype(F32)
    gl_ref[...] = total.T if z.direct else total
    count(rrecv.at[pl.ds(0, z.n - 1)], gr_recv)
    total = rrecv[0:z.mp].astype(F32)
    for dd in range(1, z.dp):
        total = total + rrecv[dd * z.mp:(dd + 1) * z.mp].astype(F32)
    gr_ref[...] = total.reshape(z.blocks, z.orow).T if z.direct else total
    count(lsend.at[pl.ds(0, z.dp - 1)], gl_send)
    count(rsend.at[pl.ds(0, z.n - 1)], gr_send)


def split_kernel(z, x_hbm, cot_hbm, rw_hbm, lw_hbm, act, gr_ref, gl_ref,
                 xfull, x2, cot, both_v, rwt, lwt, rg, rg2, lg, p1, p2, wt, wt2, lt, gracc, glacc,
                 isend, irecv, dsend, drecv, turn, esend, erecv, fsend, frecv, rsend, rrecv, final,
                 lsend, lrecv,
                 x_recv, x_send, x_local, c_local, w_local, i_send, i_recv, d_recv,
                 row_send, pair_send, gr_recv,
                 e_recv, f_recv, rw_recv, rb_recv, lw_recv, gl_recv, ra_recv, met):
    d, p = lax.axis_index("dp"), lax.axis_index("mp")
    me = d * z.mp + p
    core = lax.rem(p, 2)
    partner = p + 1 - 2 * core
    chip = p // 2
    chips = z.mp // 2
    n1, n2, tc = z.n1, z.n2, z.tc
    first = n1 * tc

    across_chip = lax.rem(chip + 1, chips) * 2
    same, other = across_chip + core, across_chip + 1 - core

    barrier = pltpu.get_barrier_semaphore()
    if z.cube:
        for s in range(1, z.mp):
            pl.semaphore_signal(barrier, inc=1, device_id=(d, lax.rem(p + s, z.mp)), device_id_type=MESH)
        for r in range(z.rounds):
            pl.semaphore_signal(barrier, inc=1, device_id=(across(d, r), p), device_id_type=MESH)
        near = z.mp - 1 + z.rounds
    else:
        @pl.loop(1, z.n)
        def _(s):
            o = lax.rem(me + s, z.n)
            pl.semaphore_signal(barrier, inc=1, device_id=(o // z.mp, lax.rem(o, z.mp)), device_id_type=MESH)
        near = z.n - 1

    def rows(c):
        return pl.ds(pl.multiple_of(c * tc, tc), tc)

    def later(c):
        return pl.ds(pl.multiple_of(first + c * tc, tc), tc)

    def local_x(part):
        span = pl.ds(0, tc) if part == 0 else pl.ds(tc, first - tc)
        return pltpu.make_async_copy(x_hbm.at[span], xfull.at[p, span], x_local.at[part])

    local_x2 = pltpu.make_async_copy(x_hbm.at[pl.ds(first, n2 * tc)], x2, c_local)
    local_c = pltpu.make_async_copy(cot_hbm, cot, c_local)

    def send_chunk(c, source, kind, target):
        return pltpu.make_async_remote_copy(
            src_ref=xfull.at[source, rows(c)], dst_ref=xfull.at[source, rows(c)],
            send_sem=x_send, recv_sem=x_recv.at[kind, c],
            device_id=(d, target), device_id_type=MESH)

    def each_mp(send):
        send(same)
        send(other)
        send(partner)

    def send_inner(c, q):
        pltpu.make_async_remote_copy(
            src_ref=isend.at[q, rows(c)], dst_ref=irecv.at[p, rows(c)],
            send_sem=i_send, recv_sem=i_recv.at[c],
            device_id=(d, q), device_id_type=MESH).start()

    def send_dinner(c, jg, sem, q):
        pltpu.make_async_remote_copy(
            src_ref=dsend.at[jg, q, rows(c)], dst_ref=drecv.at[jg, p, rows(c)],
            send_sem=i_send, recv_sem=d_recv.at[sem],
            device_id=(d, q), device_id_type=MESH).start()

    def send_first(q):
        pltpu.make_async_remote_copy(
            src_ref=fsend.at[q], dst_ref=frecv.at[p], send_sem=pair_send, recv_sem=f_recv,
            device_id=(d, q), device_id_type=MESH).start()

    def send_rows(src, dst, recv, send=row_send):
        @pl.loop(1, z.dp)
        def _(s):
            o = lax.rem(d + s, z.dp)
            pltpu.make_async_remote_copy(
                src_ref=src(o), dst_ref=dst, send_sem=send, recv_sem=recv,
                device_id=(o, p), device_id_type=MESH).start()

    def count(ref, sem):
        pltpu.make_async_copy(ref, ref, sem).wait()

    def others(ref):
        return ref.at[pl.ds(0, z.mp - 1)]

    local_x(0).start()
    local_r = pltpu.make_async_copy(rw_hbm, both_v.at[0], w_local)
    local_r.start()
    local_l = pltpu.make_async_copy(lw_hbm, both_v.at[1], w_local)
    local_l.start()

    def send_x(c):
        send_chunk(c, p, 0, same).start()
        send_chunk(c, p, 1, partner).start()

    local_x(0).wait()
    local_x(1).start()
    pl.semaphore_wait(barrier, near)
    send_x(0)
    pltpu.make_async_copy(both_v, both_v, w_local).wait()
    shape = (z.mp * z.pad, z.bs)
    a, b = iota(shape, 0), iota(shape, 1)
    wide = ones_where((a % z.pad < z.own) & (b == (a // z.pad) * z.own + a % z.pad))
    rwt[...] = dot_nt(wide, both_v[0]).astype(BF).reshape(z.mp, z.pad, z.orow)
    shape = (z.bs, z.bs)
    lwt[...] = dot_nt(ones_where(iota(shape, 0) == iota(shape, 1)), both_v[1]).astype(BF)
    rg[me] = rwt[p]
    rg2[d] = rwt[...]
    lg[d] = lwt[...]
    for s in range(1, z.mp):
        q = lax.rem(p + s, z.mp)
        pltpu.make_async_remote_copy(
            src_ref=rwt.at[q], dst_ref=rg.at[me], send_sem=pair_send, recv_sem=ra_recv,
            device_id=(d, q), device_id_type=MESH).start()

    local_x(1).wait()

    @pl.loop(1, n1)
    def _(c):
        send_x(c)

    if z.cube:
        for r in range(z.rounds):
            pl.semaphore_signal(met.at[r], inc=1, device_id=(across(d, r), p), device_id_type=MESH)
            pl.semaphore_wait(met.at[r], 1)

    local_x2.start()
    local_c.start()
    send_rows(lambda o: rwt, rg2.at[d], rb_recv)
    send_rows(lambda o: lwt, lg.at[d], lw_recv)
    count(others(rg), ra_recv)
    mine = rg.at[pl.ds(d * z.mp, z.mp)]
    send_rows(lambda o: mine, mine, rw_recv)

    for dd in range(z.dp):
        shape = (z.orow, z.feat)
        a, b = iota(shape, 0), iota(shape, 1)
        source = (b // z.bs) * z.rows + (b % z.bs) - dd * z.rows
        inside = (b % z.bs) // z.rows == dd
        p1[dd] = ones_where(inside & (a == source))
        shape = (z.orow, z.blocks * z.own)
        a, b = iota(shape, 0), iota(shape, 1)
        jg = b // z.rh
        i_all = (b % z.rh) // z.jl
        j = jg * z.jl + b % z.jl
        inside = i_all // z.rows == dd
        p2[dd] = ones_where(inside & (a == j * z.rows + i_all % z.rows))
    for a in range(z.quads):
        shape = (256, 256)
        u, v = iota(shape, 0), iota(shape, 1)
        owner = (u % z.bs) // z.rows
        slot = (v % 128) // z.unit
        match = (u // z.bs == (v % z.unit) // z.rows) & (u % z.rows == v % z.rows)
        turn[a] = ones_where(match & (owner // z.slots == v // 128) & ((owner + a) % z.slots == slot))
    gracc[...] = jnp.zeros_like(gracc)
    glacc[...] = jnp.zeros_like(glacc)

    def expand(blocks, target):
        right = None
        for dd in range(z.dp):
            part = dot_nn(blocks(dd).reshape(z.mp * z.pad, z.orow), p1[dd])
            right = part if right is None else right + part
        right = right.astype(BF)
        for g in range(z.mp):
            shape = (z.ng, z.mp * z.pad)
            a, b = iota(shape, 0), iota(shape, 1)
            pick = ones_where(b == g * z.pad + (a // z.nj) * z.jl + a % z.jl)
            piece = dot_nn(pick, right)
            shape = (z.ng, z.feat)
            keep = (iota(shape, 0) // z.jl) % z.own == iota(shape, 1) // z.bs
            target[g] = jnp.where(keep, piece, 0.0).astype(BF)

    count(rg2.at[pl.ds(0, z.dp - 1)], rb_recv)
    expand(lambda dd: rg2[dd], wt2)

    count(xfull.at[pl.ds(0, 3)], c_local)

    @pl.loop(0, n2)
    def _(c):
        own = x2[rows(c)]
        for q in range(z.mp):
            isend[q, rows(c)] = dot_nt(own, wt2[q]).astype(BF)
        each_mp(functools.partial(send_inner, c))
        irecv[p, rows(c)] = isend[p, rows(c)]
        for a in range(z.quads):
            cols = slice(a * 256, (a + 1) * 256)
            x2[rows(c), cols] = dot_nn(own[:, cols], turn[a]).astype(BF)

    def pass_on(c):
        send_chunk(c, same, 0, partner).wait_recv()
        send_chunk(c, same, 1, partner).start()

    for c in range(z.early):
        pass_on(c)

    count(lg.at[pl.ds(0, z.dp - 1)], lw_recv)
    left = None
    for dd in range(z.dp):
        part = dot_nn(lg[dd], p2[dd])
        left = part if left is None else left + part
    left = left.astype(BF)
    shape = (z.fj, z.bs)
    spread = ones_where(iota(shape, 0) % z.bs == iota(shape, 1))
    for jg in range(z.jg):
        piece = dot_nn(spread, left[:, jg * z.rh:(jg + 1) * z.rh])
        keep = iota((z.fj, z.rh), 0) // z.bs == iota((z.fj, z.rh), 1) % z.jl
        lt[jg] = jnp.where(keep, piece, 0.0).astype(BF)

    count(rg.at[pl.ds(0, z.n - z.mp)], rw_recv)
    expand(lambda dd: rg[dd * z.mp:(dd + 1) * z.mp], wt)

    def layer(inner, r):
        back = []
        for jg in range(z.jg):
            mixed = join([v[:, jg * z.nj:(jg + 1) * z.nj] for v in inner])
            pre = dot_nt(mixed, lt[jg])
            cdf = 0.5 * (1.0 + lax.erf(pre * 0.7071067811865476))
            slope = cdf + pre * (jnp.exp(-0.5 * pre * pre) * 0.3989422804014327)
            cols = pl.ds(jg * z.fj, z.fj)
            act[r, cols] = (pre * cdf).astype(BF)
            dpre = (cot[r, cols].astype(F32) * slope).astype(BF)
            glacc[jg] += dot_tn(dpre, mixed)
            back.append(dot_nn(dpre, lt[jg]).astype(BF))
        return back

    @pl.loop(0, n1)
    def _(c):
        @pl.when(c >= z.early)
        def _():
            pass_on(c)

        count(xfull.at[pl.ds(0, 2), rows(c)], x_recv.at[1, c])
        r = rows(c)
        xs = [xfull[g, r] for g in range(z.mp)]
        back = layer([dot_nt(xs[g], wt[g]).astype(BF) for g in range(z.mp)], r)
        for g in range(z.mp):
            dinner = join([v[:, g * z.nj:(g + 1) * z.nj] for v in back])
            gracc[g] += dot_tn(dinner, xs[g])

    per = 128 // z.bs
    lane = iota((z.jl, 128), 1) // z.bs

    def diagonal(tile):
        parts = []
        for v in range(z.own // per):
            piece = tile(v * per, v)
            for w in range(1, per):
                piece = jnp.where(lane == w, tile(v * per + w, v), piece)
            parts.append(piece)
        return join(parts)

    pieces = []
    for g in range(z.mp):
        for jg in range(z.jg):
            pieces.append(diagonal(lambda i, v: gracc[
                g, jg * z.nj + i * z.jl:jg * z.nj + (i + 1) * z.jl, v * 128:(v + 1) * 128]))
    pieces = join(pieces, axis=0).astype(BF)
    for dd in range(z.dp):
        esend[dd] = dot_nt(pieces, p1[dd]).astype(BF)

    send_rows(lambda o: esend.at[o], erecv.at[d], e_recv)
    erecv[d] = esend[d]

    @pl.loop(0, n2)
    def _(c):
        r = rows(c)
        count(irecv.at[pl.ds(0, z.mp - 1), r], i_recv.at[c])
        back = layer([irecv[g, r] for g in range(z.mp)], later(c))
        for jg in range(z.jg):
            for g in range(z.mp):
                dsend[jg, g, r] = back[jg][:, g * z.nj:(g + 1) * z.nj]
            drecv[jg, p, r] = dsend[jg, p, r]
        send_dinner(c, 0, 2, same)
        send_dinner(c, 0, 2, other)
        send_dinner(c, 0, 0, partner)

    @pl.loop(0, n2)
    def _(c):
        send_dinner(c, 1, 3, across_chip)
        send_dinner(c, 1, 1, partner)

    @pl.loop(0, n2 - 1)
    def _(c):
        send_dinner(c, 1, 4, across_chip + 1)

    send_dinner(n2 - 1, 1, 5, across_chip + 1)

    shape = (z.bs, z.fj)
    fold = ones_where(iota(shape, 1) % z.bs == iota(shape, 0))
    lefts = []
    for jg in range(z.jg):
        keep = iota((z.fj, z.rh), 0) // z.bs == iota((z.fj, z.rh), 1) % z.jl
        lefts.append(dot_nn(fold, jnp.where(keep, glacc[jg], 0.0).astype(BF)).astype(BF))
    left = join(lefts)
    for dd in range(z.dp):
        lsend[dd] = dot_nt(left, p2[dd]).astype(BF)

    send_rows(lambda o: lsend.at[o], lrecv.at[d], gl_recv)
    lrecv[d] = lsend[d]

    count(erecv.at[pl.ds(0, z.dp - 1)], e_recv)
    total = erecv[0].astype(F32)
    for dd in range(1, z.dp):
        total = total + erecv[dd].astype(F32)
    fsend[...] = total.astype(BF).reshape(z.mp, z.own, z.orow)
    each_mp(send_first)
    frecv[p] = fsend[p]

    shape = (z.jl, 128)
    block_of = (iota(shape, 1) % z.unit) // z.rows
    slot_of = iota(shape, 1) // z.unit

    def pick(options, which):
        out = options[0]
        for w in range(1, len(options)):
            out = jnp.where(which == w, options[w], out)
        return out

    def owned(jg, sources, lo, hi):
        turned = [drecv[jg, q, lo * tc:hi * tc].T for q in sources]
        m = z.quad * z.jl
        tiles = []
        for a in range(z.quads):
            lhs = join([t[a * m:(a + 1) * m] for t in turned], axis=0)
            full = dot_nn(lhs, x2[lo * tc:hi * tc, a * 256:(a + 1) * 256])
            tiles.append([[pick([full[k * m + w * z.jl:k * m + (w + 1) * z.jl, h * 128:(h + 1) * 128]
                                 for w in range(z.quad)], block_of) for k in range(len(sources))] for h in range(256 // 128)])
        out = []
        for dd in range(z.dp):
            h, t = dd // z.slots, dd % z.slots
            out.append(join([pick([tiles[(w - t) % z.slots][h][k] for w in range(z.slots)], slot_of)
                             for k in range(len(sources))], axis=0))
        return out

    def exchange(unit, blocks):
        for dd in range(z.dp):
            rsend[unit, dd] = blocks[dd].astype(BF)
        for s in range(1, z.dp):
            o = lax.rem(d + s, z.dp)
            pltpu.make_async_remote_copy(
                src_ref=rsend.at[unit, o], dst_ref=rrecv.at[unit, d],
                send_sem=row_send, recv_sem=gr_recv.at[unit // 3],
                device_id=(o, p), device_id_type=MESH).start()
        rrecv[unit, d] = rsend[unit, d]

    whole = (0, n2)
    near_pair = (chip * 2, chip * 2 + 1)
    far_pair = (across_chip, across_chip + 1)
    for jg in range(2):
        count(drecv.at[jg, 0], d_recv.at[jg])
        exchange(jg, owned(jg, near_pair, *whole))
    count(drecv.at[0, pl.ds(0, 2)], d_recv.at[2])
    exchange(2, owned(0, far_pair, *whole))

    @pl.when(core == 0)
    def _():
        count(drecv.at[1, pl.ds(0, 2)], d_recv.at[3])
        exchange(3, owned(1, far_pair, *whole))

    @pl.when(core == 1)
    def _():
        count(drecv.at[1, pl.ds(0, 2), pl.ds(0, (n2 - 1) * tc)], d_recv.at[4])
        most = owned(1, far_pair, 0, n2 - 1)
        count(drecv.at[1, pl.ds(0, 2), pl.ds(0, tc)], d_recv.at[5])
        last = owned(1, far_pair, n2 - 1, n2)
        exchange(3, [u + v for u, v in zip(most, last)])

    count(xfull.at[pl.ds(0, 3)], x_send)
    count(xfull.at[pl.ds(0, z.mp - 1), pl.ds(0, 2 * n2 * tc * z.ng // z.feat)], i_send)
    count(rg.at[pl.ds(0, 2 * (z.mp - 1))], pair_send)
    count(lrecv.at[pl.ds(0, z.dp - 1)], gl_recv)
    total = lrecv[0].astype(F32)
    for dd in range(1, z.dp):
        total = total + lrecv[dd].astype(F32)
    gl_ref[...] = total.T
    count(others(frecv), f_recv)
    spin = lax.rem(128 - lax.rem(d, z.slots) * z.unit, 128)

    def gather(ref, sources, jg):
        total = ref[0].astype(F32)
        for dd in range(1, z.dp):
            total = total + ref[dd].astype(F32)
        total = pltpu.roll(total, spin, 1)
        for k, q in enumerate(sources):
            piece = total[k * z.jl:(k + 1) * z.jl]
            final[q, jg] = piece + frecv[q, jg * z.jl:(jg + 1) * z.jl].astype(F32)

    count(rrecv.at[pl.ds(0, 3), pl.ds(0, z.dp - 1)], gr_recv.at[0])
    gather(rrecv.at[0], near_pair, 0)
    gather(rrecv.at[1], near_pair, 1)
    gather(rrecv.at[2], far_pair, 0)
    count(rrecv.at[3, pl.ds(0, z.dp - 1)], gr_recv.at[1])
    gather(rrecv.at[3], far_pair, 1)
    gr_ref[...] = final[...].reshape(z.blocks, z.orow).T
    count(x2.at[pl.ds(0, (z.dp - 1) * (5 * z.blocks + 8 * z.jl) * z.orow // z.feat)], row_send)


def split_scratch(z):
    dma = pltpu.SemaphoreType.DMA
    return [
        pltpu.VMEM((z.mp, z.n1 * z.tc, z.feat), BF),
        pltpu.VMEM((z.n2 * z.tc, z.feat), BF),
        pltpu.VMEM((z.tok, z.feat), BF),
        pltpu.VMEM((2, z.orow, z.bs), BF),
        pltpu.VMEM((z.mp, z.pad, z.orow), BF),
        pltpu.VMEM((z.bs, z.orow), BF),
        pltpu.VMEM((z.n, z.pad, z.orow), BF),
        pltpu.VMEM((z.dp, z.mp, z.pad, z.orow), BF),
        pltpu.VMEM((z.dp, z.bs, z.orow), BF),
        pltpu.VMEM((z.dp, z.orow, z.feat), BF),
        pltpu.VMEM((z.dp, z.orow, z.blocks * z.own), BF),
        pltpu.VMEM((z.mp, z.ng, z.feat), BF),
        pltpu.VMEM((z.mp, z.ng, z.feat), BF),
        pltpu.VMEM((z.jg, z.fj, z.rh), BF),
        pltpu.VMEM((z.mp, z.ng, z.feat), F32),
        pltpu.VMEM((z.jg, z.fj, z.rh), F32),
        pltpu.VMEM((z.mp, z.n2 * z.tc, z.ng), BF),
        pltpu.VMEM((z.mp, z.n2 * z.tc, z.ng), BF),
        pltpu.VMEM((z.jg, z.mp, z.n2 * z.tc, z.nj), BF),
        pltpu.VMEM((z.jg, z.mp, z.n2 * z.tc, z.nj), BF),
        pltpu.VMEM((z.quads, 256, 256), BF),
        pltpu.VMEM((z.dp, z.blocks, z.orow), BF),
        pltpu.VMEM((z.dp, z.blocks, z.orow), BF),
        pltpu.VMEM((z.mp, z.own, z.orow), BF),
        pltpu.VMEM((z.mp, z.own, z.orow), BF),
        pltpu.VMEM((4, z.dp, 2 * z.jl, z.orow), BF),
        pltpu.VMEM((4, z.dp, 2 * z.jl, z.orow), BF),
        pltpu.VMEM((z.mp, z.jg, z.jl, z.orow), F32),
        pltpu.VMEM((z.dp, z.bs, z.orow), BF),
        pltpu.VMEM((z.dp, z.bs, z.orow), BF),
        dma((2, z.n1)),
        dma,
        dma((2,)),
        dma, dma, dma,
        dma((z.n2,)),
        dma((6,)),
        dma, dma,
        dma((2,)),
        dma, dma, dma, dma, dma, dma, dma,
        pltpu.SemaphoreType.REGULAR((max(1, z.rounds),)),
    ]


def store(*refs):
    sems = refs[6]
    copies = [pltpu.make_async_copy(refs[k], refs[k + 3], sems.at[k]) for k in range(3)]
    for copy in copies:
        copy.start()
    for copy in copies:
        copy.wait()


def shards(z, tokens, right_weight, left_weight, cotangent):
    rw = right_weight.reshape(z.orow, z.bs)
    lw = left_weight.reshape(z.orow, z.bs)
    hbm = pl.BlockSpec(memory_space=pltpu.HBM)
    vmem = pl.BlockSpec(memory_space=pltpu.VMEM)
    dma = pltpu.SemaphoreType.DMA
    act, gr, gl = pl.pallas_call(
        functools.partial(split_kernel if z.split else kernel, z),
        out_shape=(
            pltpu.VMEM((z.tok, z.feat), BF),
            pltpu.VMEM((z.orow, z.bs) if z.direct else (z.mp, z.pad, z.orow), F32),
            pltpu.VMEM((z.orow, z.bs) if z.direct else (z.bs, z.orow), F32),
        ),
        in_specs=[hbm] * 4,
        out_specs=(vmem, vmem, vmem),
        scratch_shapes=split_scratch(z) if z.split else [
            pltpu.VMEM((z.mp, z.tok, z.feat), BF),
            pltpu.VMEM((z.tok, z.feat), BF),
            pltpu.VMEM((z.orow, z.bs), BF),
            pltpu.VMEM((z.orow, z.bs), BF),
            pltpu.VMEM((z.mp, z.pad, z.orow), BF),
            pltpu.VMEM((z.bs, z.orow), BF),
            pltpu.VMEM((z.n, z.pad, z.orow), BF),
            pltpu.VMEM((z.dp, z.bs, z.orow), BF),
            pltpu.VMEM((z.dp, z.orow, z.feat), BF),
            pltpu.VMEM((z.dp, z.orow, z.blocks * z.own), BF),
            pltpu.VMEM((z.groups, z.ng, z.kg), BF),
            pltpu.VMEM((z.jg, z.fj, z.rh), BF),
            pltpu.VMEM((z.groups, z.ng, z.kg), F32),
            pltpu.VMEM((z.jg, z.fj, z.rh), F32),
            pltpu.VMEM((z.n, z.pad, z.orow), BF),
            pltpu.VMEM((z.n, z.pad, z.orow), BF),
            pltpu.VMEM((z.dp, z.bs, z.orow), BF),
            pltpu.VMEM((z.dp, z.bs, z.orow), BF),
            dma((z.mp, z.parts)),
            dma((z.mp, z.parts)),
            dma((z.parts,)),
            dma((z.parts,)),
            dma((2,)),
            dma, dma, dma, dma, dma, dma, dma, dma, dma, dma,
            pltpu.SemaphoreType.REGULAR((max(1, z.rounds),)),
        ],
        compiler_params=pltpu.CompilerParams(
            collective_id=0, has_side_effects=True, vmem_limit_bytes=61 * 1024 * 1024),
    )(tokens, cotangent, rw, lw)
    act, gr, gl = pl.pallas_call(
        store,
        out_shape=[jax.ShapeDtypeStruct(v.shape, v.dtype) for v in (act, gr, gl)],
        in_specs=[vmem] * 3,
        out_specs=[hbm] * 3,
        scratch_shapes=[dma((3,))],
        compiler_params=pltpu.CompilerParams(vmem_limit_bytes=1024 * 1024),
    )(act, gr, gl)
    if z.direct:
        return act, gr.reshape(z.own, z.rows, z.bs), gl.reshape(z.own, z.rows, z.bs)
    gr = gr[:, :z.own].reshape(z.mp * z.own, z.own, z.rows).transpose(1, 2, 0)
    gl = gl.reshape(z.bs, z.own, z.rows).transpose(1, 2, 0)
    return act, gr, gl


def solution(mesh):
    n_dp, n_mp = mesh.shape["dp"], mesh.shape["mp"]

    def step(tokens, right_weight, left_weight, cotangent):
        z = Sizes(n_dp, n_mp, tokens.shape[0] // n_dp, tokens.shape[1] // n_mp, right_weight.shape[1])
        return jax.shard_map(
            functools.partial(shards, z),
            mesh=mesh,
            in_specs=(P("dp", "mp"), P("mp", "dp", None), P("mp", "dp", None), P("dp", "mp")),
            out_specs=(P("dp", "mp"), P("mp", "dp", None), P("mp", "dp", None)),
            check_vma=False,
        )(tokens, right_weight, left_weight, cotangent)

    return step
```
